128 devices in a mesh: rx: 16 (over x, y), ry: 8 (over z, core).
Axes of the slice: x: 4, y: 4, z: 4, core: 2. Of those that a mesh axis runs over, the one named last changes fastest.
Arguments:
- rhs: float32 [16384, 128], P(('rx', 'ry')), may hold values from -6 to 6
- a_diag: bfloat16 [16384, 128, 128], P(('rx', 'ry'))
- a_pair: bfloat16 [16384, 128, 128], P(('rx', 'ry')), may hold values from -0.25 to 0.25
- a_far: bfloat16 [16384, 2, 128, 128], P(('rx', 'ry')), may hold values from -0.25 to 0.25
- approx_inv: bfloat16 [16384, 128, 128], P(('rx', 'ry'))
- prolong: bfloat16 [16384, 128, 128], P(('rx', 'ry'))
- col_index: int32 [16384, 2], P(('rx', 'ry')), may hold values from 0 to 16383, as said below
- partner: int32 [8192], P(('rx', 'ry')), may hold values from 1 to 16383, as said below
- odd_owner: int32 [8192], P(('rx', 'ry')), may hold values from 0 to 8191, as said below
Outputs:
- fine: float32 [16384, 128], P(('rx', 'ry'))
- coarse_blocks: bfloat16 [8192, 128, 128], P(('rx', 'ry'))
- coarse_residual: float32 [8192, 128], P(('rx', 'ry'))
The draws below stay inside these ranges and needn't reach their ends.
Inputs may be any that keep to these rules, and one draw needn't show every extreme that they name: partner[c] is an odd fine row on another device with the same ry index as coarse row c's device (coarse row c stands on device c // 64, fine row i on device i // 128); every odd fine row is named once; the odd rows of each device go to exactly 8 devices, 8 rows to each. odd_owner[o] is the coarse row c with partner[c] = 2o + 1. col_index[i,0] is a block row of a device with the same ry index as row i's device; col_index[i,1] a block row of the device with the same rx index whose ry index is one more or one less, wrapping.
All inputs are finite; a program needn't handle non-finite values.
Results may differ from the reference program's by a relative error of at most 0.0065.
Values may be sent and summed in bfloat16 or wider, within the bound.
No kernel may reach another device: no remote copies, remote signals or barrier semaphores. Data moves between devices by JAX's collectives and lax.ppermute only.
A program may use at most 128 MiB of HBM per device.

```python
import math
import jax
import jax.numpy as jnp
from jax import lax

B = 128
BR_DEV = 128
SWEEPS = 2
OFFS = 8
CR_DEV = 64
CAP = 8
NB = 16384
NC = 8192
N_RX = 16
N_RY = 8


def noise_blocks(key):
    return jax.random.normal(key, (NB, B, B), jnp.float32)


def matched(key):
    base_key = jax.random.fold_in(key, 7)
    devices = N_RX * N_RY
    key_set = jax.random.split(base_key, 3)
    line_keys = jax.random.split(key_set[0], N_RY)
    offsets = jax.vmap(lambda item_key: jax.random.permutation(item_key, N_RX - 1))(line_keys).astype(jnp.int32)[:, :OFFS] + 1
    source_order = jax.vmap(lambda item_key: jax.random.permutation(item_key, CR_DEV))(jax.random.split(key_set[1], devices)).astype(jnp.int32)
    slot_order = jax.vmap(lambda item_key: jax.random.permutation(item_key, CR_DEV))(jax.random.split(key_set[2], devices)).astype(jnp.int32)
    device_ids = jnp.arange(devices, dtype=jnp.int32)[:, None]
    line_index = device_ids // N_RY
    column_index = device_ids % N_RY
    group_index = slot_order // CAP
    rank_index = slot_order % CAP
    source_line = (line_index - offsets[column_index, group_index]) % N_RX
    source_dev = source_line * N_RY + column_index
    local_odd = source_order[source_dev, group_index * CAP + rank_index]
    partner_ids = (source_dev * BR_DEV + 2 * local_odd + 1).reshape(-1).astype(jnp.int32)
    coarse_ids = (device_ids * CR_DEV + jnp.arange(CR_DEV, dtype=jnp.int32)[None, :]).reshape(-1).astype(jnp.int32)
    owner_ids = jnp.zeros((NC,), jnp.int32).at[(source_dev * CR_DEV + local_odd).reshape(-1)].set(coarse_ids)
    return (partner_ids, owner_ids)


def draw_partner(key, part):
    return matched(key)[0]


def draw_odd_owner(key, part):
    return matched(key)[1]


def draw_col_index(key, part):
    key_set = jax.random.split(jax.random.fold_in(key, 11), 4)
    row_ids = jnp.arange(NB, dtype=jnp.int32)
    device_ids = row_ids // BR_DEV
    line_index = device_ids // N_RY
    column_index = device_ids % N_RY
    far_line = jax.random.randint(key_set[0], (NB,), 0, N_RX, jnp.int32)
    far_local = jax.random.randint(key_set[1], (NB,), 0, BR_DEV, jnp.int32)
    first_col = (far_line * N_RY + column_index) * BR_DEV + far_local
    direction = jax.random.randint(key_set[2], (NB,), 0, 2, jnp.int32) * 2 - 1
    side_column = (column_index + direction) % N_RY
    side_local = jax.random.randint(key_set[3], (NB,), 0, BR_DEV, jnp.int32)
    second_col = (line_index * N_RY + side_column) * BR_DEV + side_local
    return jnp.stack([first_col, second_col], axis=1).astype(jnp.int32)


def draw_a_diag(key, part):
    key_set = jax.random.split(jax.random.fold_in(key, 21), 2)
    scales = jax.random.uniform(key_set[1], (NB, B), jnp.float32, 3.5, 5.0)
    identity = jnp.eye(B, dtype=jnp.float32)
    return (noise_blocks(key_set[0]) / B ** 0.5 + identity[None, :, :] * scales[:, :, None]).astype(jnp.bfloat16)


def draw_approx_inv(key, part):
    identity = jnp.eye(B, dtype=jnp.float32)
    return (0.25 * identity[None, :, :] + 0.08 * noise_blocks(jax.random.fold_in(key, 31)) / B ** 0.5).astype(jnp.bfloat16)


def draw_prolong(key, part):
    identity = jnp.eye(B, dtype=jnp.float32)
    return (identity[None, :, :] + 0.5 * noise_blocks(jax.random.fold_in(key, 41)) / B ** 0.5).astype(jnp.bfloat16)


def steps_of(own_key, extent, cuts, least, top_value):
    factor_of, own = 1.0, jax.random.fold_in(own_key, 6)
    for position, shards_of in cuts:
        heights = jnp.exp(jax.random.uniform(jax.random.fold_in(own, position), (shards_of,), jnp.float32, least / len(cuts), top_value / len(cuts)))
        factor_of = factor_of * jnp.repeat(heights, extent[position] // shards_of).reshape([-1 if axis == position else 1 for axis in range(len(extent))])
    return factor_of


def bell_draw(key, extent, scale, reach, cuts=(), held_as=jnp.bfloat16):
    drawn = jax.random.normal(key, extent, jnp.float32) * scale
    if len(cuts) > 0:
        drawn = steps_of(key, extent, cuts, -0.22, 0.18) * drawn
    return jnp.clip(drawn, min=-reach, max=reach).astype(held_as)


def setup_inputs(seed: int = 0) -> dict:
    seeds = jax.random.split(jax.random.key(seed), 10)
    rhs = bell_draw(seeds[0], (NB, B), 1.0, 6.0, ((0, 128),), jnp.float32)
    a_diag = draw_a_diag(jax.random.fold_in(seeds[9], 71), 0)
    a_pair = bell_draw(seeds[2], (NB, B, B), (4 * B) ** -0.5, 0.25, ((0, 128),))
    a_far = bell_draw(seeds[3], (NB, 2, B, B), (4 * B) ** -0.5, 0.25, ((0, 128),))
    approx_inv = draw_approx_inv(jax.random.fold_in(seeds[9], 71), 0)
    prolong = draw_prolong(jax.random.fold_in(seeds[9], 71), 0)
    col_index = draw_col_index(jax.random.fold_in(seeds[9], 71), 0)
    partner = draw_partner(jax.random.fold_in(seeds[9], 71), 0)
    odd_owner = draw_odd_owner(jax.random.fold_in(seeds[9], 71), 0)
    return dict(rhs=rhs, a_diag=a_diag, a_pair=a_pair, a_far=a_far, approx_inv=approx_inv, prolong=prolong, col_index=col_index, partner=partner, odd_owner=odd_owner)


OMEGA = 0.7
THETA = 0.08


def mat_vec(matrix, vector):
    return jnp.einsum('nij,nj->ni', matrix.astype(jnp.float32), vector, precision=lax.Precision.HIGHEST)


def mat_tvec(matrix, vector):
    return jnp.einsum('nji,nj->ni', matrix.astype(jnp.float32), vector, precision=lax.Precision.HIGHEST)


def mat_mat(left_mat, right_mat):
    return jnp.einsum('nij,njk->nik', left_mat.astype(jnp.float32), right_mat.astype(jnp.float32), precision=lax.Precision.HIGHEST)


def mat_tmat(left_mat, right_mat):
    return jnp.einsum('nji,njk->nik', left_mat.astype(jnp.float32), right_mat.astype(jnp.float32), precision=lax.Precision.HIGHEST)


def rounded(values):
    return lax.optimization_barrier(values.astype(jnp.bfloat16))


def by_groups(function, amount):
    group_size = math.gcd(amount, 256)
    indices = jnp.arange(amount, dtype=jnp.int32).reshape(amount // group_size, group_size)
    mapped = lax.map(function, indices)
    return jax.tree.map(lambda tensor: tensor.reshape((amount,) + tensor.shape[2:]), mapped)


def reference(rhs, a_diag, a_pair, a_far, approx_inv, prolong, col_index, partner, odd_owner):
    mate = jnp.stack([partner, 2 * odd_owner], axis=1).reshape(NB).astype(jnp.int32)

    def operate(vector):
        def row_terms(indices):
            total = mat_vec(a_diag[indices], vector[indices])
            total = total + mat_vec(a_pair[indices], vector[mate[indices]])
            total = total + mat_vec(a_far[indices, 0], vector[col_index[indices, 0]])
            return total + mat_vec(a_far[indices, 1], vector[col_index[indices, 1]])
        return by_groups(row_terms, NB)

    iterate = jnp.zeros((NB, B), jnp.float32)
    for sweep_index in range(SWEEPS):
        defect = rhs - operate(iterate)
        iterate = iterate + OMEGA * by_groups(lambda indices: mat_vec(approx_inv[indices], defect[indices]), NB)
    residual = rhs - operate(iterate)

    def coarse_rows(indices):
        even_rows = 2 * indices
        odd_rows = partner[indices]
        first_map = prolong[even_rows]
        second_map = prolong[odd_rows]
        upper = rounded(mat_tmat(first_map, a_diag[even_rows]))
        across = rounded(mat_tmat(first_map, a_pair[even_rows]))
        lower = rounded(mat_tmat(second_map, a_diag[odd_rows]))
        behind = rounded(mat_tmat(second_map, a_pair[odd_rows]))
        inner = rounded(mat_mat(lower, second_map))
        total = mat_mat(upper, first_map) + mat_mat(across, second_map) + mat_mat(behind, first_map) + inner.astype(jnp.float32)
        blocks = rounded(total)
        restricted = mat_tvec(first_map, residual[even_rows]) + mat_tvec(second_map, residual[odd_rows])
        correction = THETA * restricted
        correction = correction + THETA * (restricted - mat_vec(blocks, correction))
        return blocks, restricted, mat_vec(first_map, correction), mat_vec(second_map, correction)

    blocks, restricted, lift_even, lift_odd = by_groups(coarse_rows, NC)
    even_ids = 2 * jnp.arange(NC, dtype=jnp.int32)
    fine = iterate.at[even_ids].add(lift_even).at[partner].add(lift_odd)
    return fine, blocks, restricted
```

```python
import functools

import jax
import jax.numpy as jnp
from jax import lax
from jax.experimental import pallas as pl
from jax.experimental.pallas import tpu as pltpu
from jax.sharding import PartitionSpec as P

OMEGA = 0.7
THETA = 0.08
B = 128
VMEM_LIMIT = 48 * 1024 * 1024
BF = jnp.bfloat16
F32 = jnp.float32

NT = (((1,), (1,)), ((), ()))
NN = (((1,), (0,)), ((), ()))
TN = (((0,), (0,)), ((), ()))


def dot(left, right, dims):
    return lax.dot_general(left, right, dims, preferred_element_type=F32)


def split(row):
    rows = lax.broadcasted_iota(jnp.int32, (8, B), 0)
    full = jnp.broadcast_to(row, (8, B))
    high = full.astype(BF).astype(F32)
    return jnp.where(rows == 0, high, jnp.where(rows == 1, full - high, 0.0)).astype(BF)


def single(row):
    rows = lax.broadcasted_iota(jnp.int32, (8, B), 0)
    return jnp.where(rows == 0, jnp.broadcast_to(row, (8, B)), 0.0).astype(BF)


def joined(product):
    return product[0:1] + product[1:2]


def params():
    return pltpu.CompilerParams(
        dimension_semantics=("arbitrary",), vmem_limit_bytes=VMEM_LIMIT
    )


def whole(shape):
    return pl.BlockSpec(shape, lambda i, *_: (0,) * len(shape))


def start_kernel(rhs, inv, out, out_low):
    for j in range(rhs.shape[0]):
        row = OMEGA * joined(dot(split(rhs[j : j + 1]), inv[j], NT))
        out[j : j + 1] = row
    out_low[...] = out[...].astype(BF)


def first_sweep(rhs, inv, group=32):
    rows = rhs.shape[0]
    return pl.pallas_call(
        start_kernel,
        out_shape=(
            jax.ShapeDtypeStruct((rows, B), F32),
            jax.ShapeDtypeStruct((rows, B), BF),
        ),
        grid=(rows // group,),
        in_specs=[
            pl.BlockSpec((group, B), lambda i: (i, 0)),
            pl.BlockSpec((group, B, B), lambda i: (i, 0, 0)),
        ],
        out_specs=(
            pl.BlockSpec((group, B), lambda i: (i, 0)),
            pl.BlockSpec((group, B), lambda i: (i, 0)),
        ),
        compiler_params=params(),
        name="first_sweep",
    )(rhs, inv)


def defect_rows(i, group, slots, rows, rhs, x, x_group, tables, low, high, diag, pair, far, tab, side, held):
    @pl.when(i == 0)
    def _():
        quarter = tables[0].shape[0]
        for k, t in enumerate(tables):
            tab[k * quarter : (k + 1) * quarter] = t[...].astype(F32)
        side[0:rows] = low[...].astype(F32)
        side[rows : 2 * rows] = high[...].astype(F32)

    for j in range(group):
        r = i * group + j
        mate = tab[pl.ds(slots[r], 1)]
        first = tab[pl.ds(slots[rows + r], 1)]
        second = side[pl.ds(slots[2 * rows + r], 1)]
        total = dot(split(x_group[j : j + 1]), diag[j], NT)
        total += dot(single(mate), pair[j], NT)
        total += dot(single(first), far[j, 0], NT)
        total += dot(single(second), far[j, 1], NT)
        held[j : j + 1] = rhs[j : j + 1] - joined(total)


def sweep_kernel(group, rows, slots, rhs, x_group, t0, t1, t2, t3, low, high, diag, pair, far, inv, out, out_low, tab, side, held):
    i = pl.program_id(0)
    defect_rows(i, group, slots, rows, rhs, None, x_group, (t0, t1, t2, t3), low, high, diag, pair, far, tab, side, held)
    for j in range(group):
        step = joined(dot(split(held[j : j + 1]), inv[j], NT))
        out[j : j + 1] = x_group[j : j + 1] + OMEGA * step
    out_low[...] = out[...].astype(BF)


def residual_kernel(group, rows, slots, sends, rhs, x_group, t0, t1, t2, t3, low, high, diag, pair, far, prol, even, packed, tab, side, held, mail):
    i = pl.program_id(0)
    defect_rows(i, group, slots, rows, rhs, None, x_group, (t0, t1, t2, t3), low, high, diag, pair, far, tab, side, held)

    @pl.when(i == 0)
    def _():
        mail[...] = jnp.zeros_like(mail)

    for j in range(group):
        value = joined(dot(split(held[j : j + 1]), prol[j], NN))
        if j % 2 == 0:
            even[j // 2 : j // 2 + 1] = value
        else:
            mail[pl.ds(sends[i * (group // 2) + j // 2], 1)] = value

    @pl.when(i == pl.num_programs(0) - 1)
    def _():
        packed[...] = mail[...].astype(BF)


def apply_specs(rows, group):
    row = pl.BlockSpec((group, B), lambda i, *_: (i, 0))
    block = pl.BlockSpec((group, B, B), lambda i, *_: (i, 0, 0))
    return [
        row,
        row,
        *[whole((4 * rows, B))] * 4,
        whole((rows, B)),
        whole((rows, B)),
        block,
        block,
        pl.BlockSpec((group, 2, B, B), lambda i, *_: (i, 0, 0, 0)),
        block,
    ]


def apply_scratch(rows, group):
    return [
        pltpu.VMEM((16 * rows, B), F32),
        pltpu.VMEM((2 * rows, B), F32),
        pltpu.VMEM((group, B), F32),
    ]


def second_sweep(slots, rhs, x, tables, low, high, diag, pair, far, inv, group=16):
    rows = rhs.shape[0]
    row = pl.BlockSpec((group, B), lambda i, *_: (i, 0))
    return pl.pallas_call(
        functools.partial(sweep_kernel, group, rows),
        out_shape=(
            jax.ShapeDtypeStruct((rows, B), F32),
            jax.ShapeDtypeStruct((rows, B), BF),
        ),
        grid_spec=pltpu.PrefetchScalarGridSpec(
            num_scalar_prefetch=1,
            grid=(rows // group,),
            in_specs=apply_specs(rows, group),
            out_specs=(row, row),
            scratch_shapes=apply_scratch(rows, group),
        ),
        compiler_params=params(),
        name="second_sweep",
    )(slots, rhs, x, *tables, low, high, diag, pair, far, inv)


def residual_pieces(slots, sends, rhs, x, tables, low, high, diag, pair, far, prol, group=16):
    rows = rhs.shape[0]
    return pl.pallas_call(
        functools.partial(residual_kernel, group, rows),
        out_shape=(
            jax.ShapeDtypeStruct((rows // 2, B), F32),
            jax.ShapeDtypeStruct((rows, B), BF),
        ),
        grid_spec=pltpu.PrefetchScalarGridSpec(
            num_scalar_prefetch=2,
            grid=(rows // group,),
            in_specs=apply_specs(rows, group),
            out_specs=(
                pl.BlockSpec((group // 2, B), lambda i, *_: (i, 0)),
                whole((rows, B)),
            ),
            scratch_shapes=apply_scratch(rows, group) + [pltpu.VMEM((rows, B), F32)],
        ),
        compiler_params=params(),
        name="residual_pieces",
    )(slots, sends, rhs, x, *tables, low, high, diag, pair, far, prol)


def odd_kernel(group, half, sends, prol, diag, pair, out, buf, sem):
    i = pl.program_id(0)

    def copy(item):
        return pltpu.make_async_copy(buf.at[item], out.at[sends[item]], sem.at[item])

    for j in range(group):
        item = i * group + j
        p = prol[j, 0]
        lower = dot(p, diag[j, 0], TN).astype(BF)
        buf[item, 0] = p
        buf[item, 1] = dot(p, pair[j, 0], TN).astype(BF)
        buf[item, 2] = dot(lower, p, NN).astype(BF)
        copy(item).start()

    @pl.when(i == pl.num_programs(0) - 1)
    def _():
        def wait(item, carry):
            copy(item).wait()
            return carry

        lax.fori_loop(0, half, wait, 0)


def odd_blocks(sends, prol, diag, pair, group=8):
    half = prol.shape[0] // 2
    odd = pl.BlockSpec((group, 1, B, B), lambda i, *_: (i, 1, 0, 0))
    return pl.pallas_call(
        functools.partial(odd_kernel, group, half),
        out_shape=jax.ShapeDtypeStruct((2 * half, 3, B, B), BF),
        grid_spec=pltpu.PrefetchScalarGridSpec(
            num_scalar_prefetch=1,
            grid=(half // group,),
            in_specs=[odd, odd, odd],
            out_specs=pl.BlockSpec(memory_space=pl.ANY),
            scratch_shapes=[
                pltpu.VMEM((half, 3, B, B), BF),
                pltpu.SemaphoreType.DMA((half,)),
            ],
        ),
        compiler_params=params(),
        name="odd_blocks",
    )(sends, *[a.reshape(half, 2, B, B) for a in (prol, diag, pair)])


def even_kernel(prol, diag, pair, out):
    for j in range(prol.shape[0]):
        p = prol[j, 0]
        out[j, 0] = dot(p, diag[j, 0], TN).astype(BF)
        out[j, 1] = dot(p, pair[j, 0], TN).astype(BF)


def even_blocks(prol, diag, pair, group=16):
    half = prol.shape[0] // 2
    even = pl.BlockSpec((group, 1, B, B), lambda i, *_: (i, 0, 0, 0))
    return pl.pallas_call(
        even_kernel,
        out_shape=jax.ShapeDtypeStruct((half, 2, B, B), BF),
        grid=(half // group,),
        in_specs=[even, even, even],
        out_specs=pl.BlockSpec((group, 2, B, B), lambda i: (i, 0, 0, 0)),
        compiler_params=params(),
        name="even_blocks",
    )(*[a.reshape(half, 2, B, B) for a in (prol, diag, pair)])


def coarse_kernel(group, half, recvs, got, mail, even, own, prol, blocks, restricted, packed, lift, buf, sem, letters, reply):
    i = pl.program_id(0)

    def copy(item):
        return pltpu.make_async_copy(got.at[recvs[item]], buf.at[item], sem.at[item])

    @pl.when(i == 0)
    def _():
        def start(item, carry):
            copy(item).start()
            return carry

        lax.fori_loop(0, half, start, 0)
        letters[...] = mail[...].astype(F32)
        reply[...] = jnp.zeros_like(reply)

    for j in range(group):
        item = i * group + j
        copy(item).wait()
    for j in range(group):
        item = i * group + j
        p = prol[j, 0]
        total = dot(own[j, 0], p, NN) + dot(own[j, 1], buf[item, 0], NN)
        total = total + dot(buf[item, 1], p, NN) + buf[item, 2].astype(F32)
        blocks[j] = total.astype(BF)
    for j in range(group):
        item = i * group + j
        slot = recvs[item]
        r = even[j : j + 1] + letters[pl.ds(slot, 1)]
        restricted[j : j + 1] = r
        c = THETA * r
        c = c + THETA * (r - joined(dot(split(c), blocks[j], NT)))
        reply[pl.ds(slot, 1)] = c
        lift[j : j + 1] = joined(dot(split(c), prol[j, 0], NT))

    @pl.when(i == pl.num_programs(0) - 1)
    def _():
        packed[...] = reply[...].astype(BF)


def coarse(recvs, got, mail, even, own, prol, group=16):
    half = even.shape[0]
    row = pl.BlockSpec((group, B), lambda i, *_: (i, 0))
    return pl.pallas_call(
        functools.partial(coarse_kernel, group, half),
        out_shape=(
            jax.ShapeDtypeStruct((half, B, B), BF),
            jax.ShapeDtypeStruct((half, B), F32),
            jax.ShapeDtypeStruct((2 * half, B), BF),
            jax.ShapeDtypeStruct((half, B), F32),
        ),
        grid_spec=pltpu.PrefetchScalarGridSpec(
            num_scalar_prefetch=1,
            grid=(half // group,),
            in_specs=[
                pl.BlockSpec(memory_space=pl.ANY),
                whole((2 * half, B)),
                row,
                pl.BlockSpec((group, 2, B, B), lambda i, *_: (i, 0, 0, 0)),
                pl.BlockSpec((group, 1, B, B), lambda i, *_: (i, 0, 0, 0)),
            ],
            out_specs=(
                pl.BlockSpec((group, B, B), lambda i, *_: (i, 0, 0)),
                row,
                whole((2 * half, B)),
                row,
            ),
            scratch_shapes=[
                pltpu.VMEM((half, 3, B, B), BF),
                pltpu.SemaphoreType.DMA((half,)),
                pltpu.VMEM((2 * half, B), F32),
                pltpu.VMEM((2 * half, B), F32),
            ],
        ),
        compiler_params=params(),
        name="coarse",
    )(recvs, got, mail, even, own, prol.reshape(half, 2, B, B))


def finish_kernel(group, sends, mail, lift, x, prol, out, letters):
    i = pl.program_id(0)

    @pl.when(i == 0)
    def _():
        letters[...] = mail[...].astype(F32)

    for j in range(group):
        e = 2 * j
        out[e : e + 1] = x[e : e + 1] + lift[j : j + 1]
        c = letters[pl.ds(sends[i * group + j], 1)]
        out[e + 1 : e + 2] = x[e + 1 : e + 2] + joined(dot(single(c), prol[j, 0], NT))


def finish(sends, mail, lift, x, prol, group=32):
    half = lift.shape[0]
    return pl.pallas_call(
        functools.partial(finish_kernel, group),
        out_shape=jax.ShapeDtypeStruct((2 * half, B), F32),
        grid_spec=pltpu.PrefetchScalarGridSpec(
            num_scalar_prefetch=1,
            grid=(half // group,),
            in_specs=[
                whole((2 * half, B)),
                pl.BlockSpec((group, B), lambda i, *_: (i, 0)),
                pl.BlockSpec((2 * group, B), lambda i, *_: (i, 0)),
                pl.BlockSpec((group, 1, B, B), lambda i, *_: (i, 1, 0, 0)),
            ],
            out_specs=pl.BlockSpec((2 * group, B), lambda i, *_: (i, 0)),
            scratch_shapes=[pltpu.VMEM((2 * half, B), F32)],
        ),
        compiler_params=params(),
        name="finish",
    )(sends, mail, lift, x, prol.reshape(half, 2, B, B))


def gather_line(block, side):
    def along_x(d):
        return [
            (x * side + y, (x + d) % side * side + y)
            for x in range(side)
            for y in range(side)
        ]

    def along_y(d):
        return [
            (x * side + y, x * side + (y + d) % side)
            for x in range(side)
            for y in range(side)
        ]

    row = [block] + [lax.ppermute(block, "rx", along_x(d)) for d in range(1, side)]
    row = jnp.concatenate(row, axis=0)
    return [row] + [lax.ppermute(row, "rx", along_y(d)) for d in range(1, side)]


def neighbours(block):
    count = lax.axis_size("ry")
    forward = [(i, (i + 1) % count) for i in range(count)]
    backward = [(target, source) for source, target in forward]
    return lax.ppermute(block, "ry", forward), lax.ppermute(block, "ry", backward)


def exchange(packed):
    line = lax.axis_size("rx")
    shape = packed.shape
    out = lax.all_to_all(
        packed.reshape((line, -1) + shape[1:]), "rx", split_axis=0, concat_axis=0, tiled=True
    )
    return out.reshape(shape)


def body(rhs, a_diag, a_pair, a_far, approx_inv, prolong, col_index, partner, odd_owner):
    rows = rhs.shape[0]
    half = rows // 2
    line_size = lax.axis_size("rx")
    side_size = lax.axis_size("ry")
    line_pos = lax.axis_index("rx")
    side_pos = lax.axis_index("ry")
    grid_side = 4
    capacity = half // (line_size // 2)
    mate = jnp.stack([partner, 2 * odd_owner], axis=1).reshape(rows)

    def line_slot(global_row):
        line = global_row // rows // side_size
        back_x = (line_pos // grid_side - line // grid_side) % grid_side
        back_y = (line_pos - line) % grid_side
        return (back_y * grid_side + back_x) * rows + global_row % rows

    side_dev = col_index[:, 1] // rows
    below = side_dev % side_size == (side_pos - 1) % side_size
    side_slot = jnp.where(below, 0, rows) + col_index[:, 1] % rows
    slots = jnp.concatenate([line_slot(mate), line_slot(col_index[:, 0]), side_slot])

    target_line = odd_owner // half // side_size
    same_target = target_line[:, None] == target_line[None, :]
    earlier = odd_owner[None, :] < odd_owner[:, None]
    sends = target_line * capacity + jnp.sum(same_target & earlier, axis=1, dtype=jnp.int32)
    source_line = partner // rows // side_size
    same_source = source_line[:, None] == source_line[None, :]
    position = jnp.arange(half, dtype=jnp.int32)
    before = position[None, :] < position[:, None]
    recvs = source_line * capacity + jnp.sum(same_source & before, axis=1, dtype=jnp.int32)

    x, x_low = first_sweep(rhs, approx_inv)
    low, high = neighbours(x_low)
    tables = gather_line(x_low, grid_side)
    leaving = odd_blocks(sends, prolong, a_diag, a_pair)
    x, x_low = second_sweep(
        slots, rhs, x, tables, low, high, a_diag, a_pair, a_far, approx_inv
    )
    low, high = neighbours(x_low)
    tables = gather_line(x_low, grid_side)
    own = even_blocks(prolong, a_diag, a_pair)
    even, mail = residual_pieces(
        slots, sends, rhs, x, tables, low, high, a_diag, a_pair, a_far, prolong
    )
    leaving, own, mail = lax.optimization_barrier((leaving, own, mail))
    got = exchange(leaving)
    mail = exchange(mail)
    blocks, restricted, reply, lift = coarse(recvs, got, mail, even, own, prolong)
    fine = finish(sends, exchange(reply), lift, x, prolong)
    return fine, blocks, restricted


def solution(mesh):
    rows = P(("rx", "ry"))
    return jax.shard_map(
        body,
        mesh=mesh,
        in_specs=(rows,) * 9,
        out_specs=(rows,) * 3,
        check_vma=False,
    )
```

```python
import functools

import jax
import jax.numpy as jnp
from jax import lax
from jax.experimental import pallas as pl
from jax.experimental.pallas import tpu as pltpu
from jax.sharding import PartitionSpec as P

OMEGA = 0.7
THETA = 0.08
B = 128
VMEM_LIMIT = 48 * 1024 * 1024
BF = jnp.bfloat16
F32 = jnp.float32

NT = (((1,), (1,)), ((), ()))
NN = (((1,), (0,)), ((), ()))
TN = (((0,), (0,)), ((), ()))


def dot(left, right, dims):
    return lax.dot_general(left, right, dims, preferred_element_type=F32)


def split(row):
    rows = lax.broadcasted_iota(jnp.int32, (8, B), 0)
    full = jnp.broadcast_to(row, (8, B))
    high = full.astype(BF).astype(F32)
    return jnp.where(rows == 0, high, jnp.where(rows == 1, full - high, 0.0)).astype(BF)


def single(row):
    rows = lax.broadcasted_iota(jnp.int32, (8, B), 0)
    return jnp.where(rows == 0, jnp.broadcast_to(row, (8, B)), 0.0).astype(BF)


def joined(product):
    return product[0:1] + product[1:2]


def params():
    return pltpu.CompilerParams(
        dimension_semantics=("arbitrary",), vmem_limit_bytes=VMEM_LIMIT
    )


def whole(shape):
    return pl.BlockSpec(shape, lambda i, *_: (0,) * len(shape))


def start_kernel(rhs, inv, out, out_low):
    for j in range(rhs.shape[0]):
        row = OMEGA * joined(dot(split(rhs[j : j + 1]), inv[j], NT))
        out[j : j + 1] = row
    out_low[...] = out[...].astype(BF)


def first_sweep(rhs, inv, group=32):
    rows = rhs.shape[0]
    return pl.pallas_call(
        start_kernel,
        out_shape=(
            jax.ShapeDtypeStruct((rows, B), F32),
            jax.ShapeDtypeStruct((rows, B), BF),
        ),
        grid=(rows // group,),
        in_specs=[
            pl.BlockSpec((group, B), lambda i: (i, 0)),
            pl.BlockSpec((group, B, B), lambda i: (i, 0, 0)),
        ],
        out_specs=(
            pl.BlockSpec((group, B), lambda i: (i, 0)),
            pl.BlockSpec((group, B), lambda i: (i, 0)),
        ),
        compiler_params=params(),
        name="first_sweep",
    )(rhs, inv)


def defect_rows(i, group, slots, rows, rhs, x, x_group, tables, low, high, diag, pair, far, tab, side, held):
    @pl.when(i == 0)
    def _():
        quarter = tables[0].shape[0]
        for k, t in enumerate(tables):
            tab[k * quarter : (k + 1) * quarter] = t[...].astype(F32)
        side[0:rows] = low[...].astype(F32)
        side[rows : 2 * rows] = high[...].astype(F32)

    for j in range(group):
        r = i * group + j
        mate = tab[pl.ds(slots[r], 1)]
        first = tab[pl.ds(slots[rows + r], 1)]
        second = side[pl.ds(slots[2 * rows + r], 1)]
        total = dot(split(x_group[j : j + 1]), diag[j], NT)
        total += dot(single(mate), pair[j], NT)
        total += dot(single(first), far[j, 0], NT)
        total += dot(single(second), far[j, 1], NT)
        held[j : j + 1] = rhs[j : j + 1] - joined(total)


def sweep_kernel(group, rows, slots, rhs, x_group, t0, t1, t2, t3, low, high, diag, pair, far, inv, out, out_low, tab, side, held):
    i = pl.program_id(0)
    defect_rows(i, group, slots, rows, rhs, None, x_group, (t0, t1, t2, t3), low, high, diag, pair, far, tab, side, held)
    for j in range(group):
        step = joined(dot(split(held[j : j + 1]), inv[j], NT))
        out[j : j + 1] = x_group[j : j + 1] + OMEGA * step
    out_low[...] = out[...].astype(BF)


def residual_kernel(group, rows, slots, sends, rhs, x_group, t0, t1, t2, t3, low, high, diag, pair, far, prol, even, packed, tab, side, held, mail):
    i = pl.program_id(0)
    defect_rows(i, group, slots, rows, rhs, None, x_group, (t0, t1, t2, t3), low, high, diag, pair, far, tab, side, held)

    @pl.when(i == 0)
    def _():
        mail[...] = jnp.zeros_like(mail)

    for j in range(group):
        value = joined(dot(split(held[j : j + 1]), prol[j], NN))
        if j % 2 == 0:
            even[j // 2 : j // 2 + 1] = value
        else:
            mail[pl.ds(sends[i * (group // 2) + j // 2], 1)] = value

    @pl.when(i == pl.num_programs(0) - 1)
    def _():
        packed[...] = mail[...].astype(BF)


def apply_specs(rows, group):
    row = pl.BlockSpec((group, B), lambda i, *_: (i, 0))
    block = pl.BlockSpec((group, B, B), lambda i, *_: (i, 0, 0))
    return [
        row,
        row,
        *[whole((4 * rows, B))] * 4,
        whole((rows, B)),
        whole((rows, B)),
        block,
        block,
        pl.BlockSpec((group, 2, B, B), lambda i, *_: (i, 0, 0, 0)),
        block,
    ]


def apply_scratch(rows, group):
    return [
        pltpu.VMEM((16 * rows, B), F32),
        pltpu.VMEM((2 * rows, B), F32),
        pltpu.VMEM((group, B), F32),
    ]


def second_sweep(slots, rhs, x, tables, low, high, diag, pair, far, inv, group=16):
    rows = rhs.shape[0]
    row = pl.BlockSpec((group, B), lambda i, *_: (i, 0))
    return pl.pallas_call(
        functools.partial(sweep_kernel, group, rows),
        out_shape=(
            jax.ShapeDtypeStruct((rows, B), F32),
            jax.ShapeDtypeStruct((rows, B), BF),
        ),
        grid_spec=pltpu.PrefetchScalarGridSpec(
            num_scalar_prefetch=1,
            grid=(rows // group,),
            in_specs=apply_specs(rows, group),
            out_specs=(row, row),
            scratch_shapes=apply_scratch(rows, group),
        ),
        compiler_params=params(),
        name="second_sweep",
    )(slots, rhs, x, *tables, low, high, diag, pair, far, inv)


def residual_pieces(slots, sends, rhs, x, tables, low, high, diag, pair, far, prol, group=16):
    rows = rhs.shape[0]
    return pl.pallas_call(
        functools.partial(residual_kernel, group, rows),
        out_shape=(
            jax.ShapeDtypeStruct((rows // 2, B), F32),
            jax.ShapeDtypeStruct((rows, B), BF),
        ),
        grid_spec=pltpu.PrefetchScalarGridSpec(
            num_scalar_prefetch=2,
            grid=(rows // group,),
            in_specs=apply_specs(rows, group),
            out_specs=(
                pl.BlockSpec((group // 2, B), lambda i, *_: (i, 0)),
                whole((rows, B)),
            ),
            scratch_shapes=apply_scratch(rows, group) + [pltpu.VMEM((rows, B), F32)],
        ),
        compiler_params=params(),
        name="residual_pieces",
    )(slots, sends, rhs, x, *tables, low, high, diag, pair, far, prol)


def odd_kernel(group, half, sends, prol, diag, pair, out, buf, sem):
    i = pl.program_id(0)

    def copy(item):
        return pltpu.make_async_copy(buf.at[item], out.at[sends[item]], sem.at[item])

    for j in range(group):
        item = i * group + j
        p = prol[j, 0]
        lower = dot(p, diag[j, 0], TN).astype(BF)
        buf[item, 0] = p
        buf[item, 1] = dot(p, pair[j, 0], TN).astype(BF)
        buf[item, 2] = dot(lower, p, NN).astype(BF)
        copy(item).start()

    @pl.when(i == pl.num_programs(0) - 1)
    def _():
        def wait(item, carry):
            copy(item).wait()
            return carry

        lax.fori_loop(0, half, wait, 0)


def odd_blocks(sends, prol, diag, pair, group=8):
    half = prol.shape[0] // 2
    odd = pl.BlockSpec((group, 1, B, B), lambda i, *_: (i, 1, 0, 0))
    return pl.pallas_call(
        functools.partial(odd_kernel, group, half),
        out_shape=jax.ShapeDtypeStruct((2 * half, 3, B, B), BF),
        grid_spec=pltpu.PrefetchScalarGridSpec(
            num_scalar_prefetch=1,
            grid=(half // group,),
            in_specs=[odd, odd, odd],
            out_specs=pl.BlockSpec(memory_space=pl.ANY),
            scratch_shapes=[
                pltpu.VMEM((half, 3, B, B), BF),
                pltpu.SemaphoreType.DMA((half,)),
            ],
        ),
        compiler_params=params(),
        name="odd_blocks",
    )(sends, *[a.reshape(half, 2, B, B) for a in (prol, diag, pair)])


def even_kernel(prol, diag, pair, out):
    for j in range(prol.shape[0]):
        p = prol[j, 0]
        out[j, 0] = dot(p, diag[j, 0], TN).astype(BF)
        out[j, 1] = dot(p, pair[j, 0], TN).astype(BF)


def even_blocks(prol, diag, pair, group=16):
    half = prol.shape[0] // 2
    even = pl.BlockSpec((group, 1, B, B), lambda i, *_: (i, 0, 0, 0))
    return pl.pallas_call(
        even_kernel,
        out_shape=jax.ShapeDtypeStruct((half, 2, B, B), BF),
        grid=(half // group,),
        in_specs=[even, even, even],
        out_specs=pl.BlockSpec((group, 2, B, B), lambda i: (i, 0, 0, 0)),
        compiler_params=params(),
        name="even_blocks",
    )(*[a.reshape(half, 2, B, B) for a in (prol, diag, pair)])


def coarse_kernel(group, half, recvs, got, mail, even, own, prol, blocks, restricted, packed, lift, buf, sem, letters, reply):
    i = pl.program_id(0)

    def copy(item):
        return pltpu.make_async_copy(got.at[recvs[item]], buf.at[item], sem.at[item])

    @pl.when(i == 0)
    def _():
        def start(item, carry):
            copy(item).start()
            return carry

        lax.fori_loop(0, half, start, 0)
        letters[...] = mail[...].astype(F32)
        reply[...] = jnp.zeros_like(reply)

    for j in range(group):
        item = i * group + j
        copy(item).wait()
    for j in range(group):
        item = i * group + j
        p = prol[j, 0]
        total = dot(own[j, 0], p, NN) + dot(own[j, 1], buf[item, 0], NN)
        total = total + dot(buf[item, 1], p, NN) + buf[item, 2].astype(F32)
        blocks[j] = total.astype(BF)
    for j in range(group):
        item = i * group + j
        slot = recvs[item]
        r = even[j : j + 1] + letters[pl.ds(slot, 1)]
        restricted[j : j + 1] = r
        c = THETA * r
        c = c + THETA * (r - joined(dot(split(c), blocks[j], NT)))
        reply[pl.ds(slot, 1)] = c
        lift[j : j + 1] = joined(dot(split(c), prol[j, 0], NT))

    @pl.when(i == pl.num_programs(0) - 1)
    def _():
        packed[...] = reply[...].astype(BF)


def coarse(recvs, got, mail, even, own, prol, group=16):
    half = even.shape[0]
    row = pl.BlockSpec((group, B), lambda i, *_: (i, 0))
    return pl.pallas_call(
        functools.partial(coarse_kernel, group, half),
        out_shape=(
            jax.ShapeDtypeStruct((half, B, B), BF),
            jax.ShapeDtypeStruct((half, B), F32),
            jax.ShapeDtypeStruct((2 * half, B), BF),
            jax.ShapeDtypeStruct((half, B), F32),
        ),
        grid_spec=pltpu.PrefetchScalarGridSpec(
            num_scalar_prefetch=1,
            grid=(half // group,),
            in_specs=[
                pl.BlockSpec(memory_space=pl.ANY),
                whole((2 * half, B)),
                row,
                pl.BlockSpec((group, 2, B, B), lambda i, *_: (i, 0, 0, 0)),
                pl.BlockSpec((group, 1, B, B), lambda i, *_: (i, 0, 0, 0)),
            ],
            out_specs=(
                pl.BlockSpec((group, B, B), lambda i, *_: (i, 0, 0)),
                row,
                whole((2 * half, B)),
                row,
            ),
            scratch_shapes=[
                pltpu.VMEM((half, 3, B, B), BF),
                pltpu.SemaphoreType.DMA((half,)),
                pltpu.VMEM((2 * half, B), F32),
                pltpu.VMEM((2 * half, B), F32),
            ],
        ),
        compiler_params=params(),
        name="coarse",
    )(recvs, got, mail, even, own, prol.reshape(half, 2, B, B))


def finish_kernel(group, sends, mail, lift, x, prol, out, letters):
    i = pl.program_id(0)

    @pl.when(i == 0)
    def _():
        letters[...] = mail[...].astype(F32)

    for j in range(group):
        e = 2 * j
        out[e : e + 1] = x[e : e + 1] + lift[j : j + 1]
        c = letters[pl.ds(sends[i * group + j], 1)]
        out[e + 1 : e + 2] = x[e + 1 : e + 2] + joined(dot(single(c), prol[j, 0], NT))


def finish(sends, mail, lift, x, prol, group=32):
    half = lift.shape[0]
    return pl.pallas_call(
        functools.partial(finish_kernel, group),
        out_shape=jax.ShapeDtypeStruct((2 * half, B), F32),
        grid_spec=pltpu.PrefetchScalarGridSpec(
            num_scalar_prefetch=1,
            grid=(half // group,),
            in_specs=[
                whole((2 * half, B)),
                pl.BlockSpec((group, B), lambda i, *_: (i, 0)),
                pl.BlockSpec((2 * group, B), lambda i, *_: (i, 0)),
                pl.BlockSpec((group, 1, B, B), lambda i, *_: (i, 1, 0, 0)),
            ],
            out_specs=pl.BlockSpec((2 * group, B), lambda i, *_: (i, 0)),
            scratch_shapes=[pltpu.VMEM((2 * half, B), F32)],
        ),
        compiler_params=params(),
        name="finish",
    )(sends, mail, lift, x, prol.reshape(half, 2, B, B))


def gather_line(block, side):
    def along_x(d):
        return [
            (x * side + y, (x + d) % side * side + y)
            for x in range(side)
            for y in range(side)
        ]

    def along_y(d):
        return [
            (x * side + y, x * side + (y + d) % side)
            for x in range(side)
            for y in range(side)
        ]

    row = [block] + [lax.ppermute(block, "rx", along_x(d)) for d in range(1, side)]
    row = jnp.concatenate(row, axis=0)
    return [row] + [lax.ppermute(row, "rx", along_y(d)) for d in range(1, side)]


def neighbours(block):
    count = lax.axis_size("ry")
    forward = [(i, (i + 1) % count) for i in range(count)]
    backward = [(target, source) for source, target in forward]
    return lax.ppermute(block, "ry", forward), lax.ppermute(block, "ry", backward)


def exchange(packed):
    line = lax.axis_size("rx")
    shape = packed.shape
    out = lax.all_to_all(
        packed.reshape((line, -1) + shape[1:]), "rx", split_axis=0, concat_axis=0, tiled=True
    )
    return out.reshape(shape)


def body(rhs, a_diag, a_pair, a_far, approx_inv, prolong, col_index, partner, odd_owner):
    rows = rhs.shape[0]
    half = rows // 2
    line_size = lax.axis_size("rx")
    side_size = lax.axis_size("ry")
    line_pos = lax.axis_index("rx")
    side_pos = lax.axis_index("ry")
    grid_side = 4
    capacity = half // (line_size // 2)
    mate = jnp.stack([partner, 2 * odd_owner], axis=1).reshape(rows)

    def line_slot(global_row):
        line = global_row // rows // side_size
        back_x = (line_pos // grid_side - line // grid_side) % grid_side
        back_y = (line_pos - line) % grid_side
        return (back_y * grid_side + back_x) * rows + global_row % rows

    side_dev = col_index[:, 1] // rows
    below = side_dev % side_size == (side_pos - 1) % side_size
    side_slot = jnp.where(below, 0, rows) + col_index[:, 1] % rows
    slots = jnp.concatenate([line_slot(mate), line_slot(col_index[:, 0]), side_slot])

    target_line = odd_owner // half // side_size
    same_target = target_line[:, None] == target_line[None, :]
    earlier = odd_owner[None, :] < odd_owner[:, None]
    sends = target_line * capacity + jnp.sum(same_target & earlier, axis=1, dtype=jnp.int32)
    source_line = partner // rows // side_size
    same_source = source_line[:, None] == source_line[None, :]
    position = jnp.arange(half, dtype=jnp.int32)
    before = position[None, :] < position[:, None]
    recvs = source_line * capacity + jnp.sum(same_source & before, axis=1, dtype=jnp.int32)

    x, x_low = first_sweep(rhs, approx_inv)
    low, high = neighbours(x_low)
    tables = gather_line(x_low, grid_side)
    leaving = odd_blocks(sends, prolong, a_diag, a_pair)
    x, x_low = second_sweep(
        slots, rhs, x, tables, low, high, a_diag, a_pair, a_far, approx_inv
    )
    low, high = neighbours(x_low)
    tables = gather_line(x_low, grid_side)
    own = even_blocks(prolong, a_diag, a_pair)
    even, mail = residual_pieces(
        slots, sends, rhs, x, tables, low, high, a_diag, a_pair, a_far, prolong
    )
    mail = exchange(mail)
    leaving, own, mail, recvs = lax.optimization_barrier((leaving, own, mail, recvs))
    got = exchange(leaving)
    blocks, restricted, reply, lift = coarse(recvs, got, mail, even, own, prolong)
    fine = finish(sends, exchange(reply), lift, x, prolong)
    return fine, blocks, restricted


def solution(mesh):
    rows = P(("rx", "ry"))
    return jax.shard_map(
        body,
        mesh=mesh,
        in_specs=(rows,) * 9,
        out_specs=(rows,) * 3,
        check_vma=False,
    )
```

```python
import functools

import jax
import jax.numpy as jnp
from jax import lax
from jax.experimental import pallas as pl
from jax.experimental.pallas import tpu as pltpu
from jax.sharding import PartitionSpec as P

OMEGA = 0.7
THETA = 0.08
ORDER = (
    *((1, 1), (3, 3), (1, 3), (3, 1), (1, 0), (2, 1), (0, 3), (3, 0)),
    *((2, 3), (0, 1), (1, 2), (3, 2), (2, 2), (0, 2), (2, 0)),
)
WINDOW = 4
B = 128
VMEM_LIMIT = 48 * 1024 * 1024
BF = jnp.bfloat16
F32 = jnp.float32

NT = (((1,), (1,)), ((), ()))
NN = (((1,), (0,)), ((), ()))
TN = (((0,), (0,)), ((), ()))


def dot(left, right, dims):
    return lax.dot_general(left, right, dims, preferred_element_type=F32)


def split(row):
    rows = lax.broadcasted_iota(jnp.int32, (8, B), 0)
    full = jnp.broadcast_to(row, (8, B))
    high = full.astype(BF).astype(F32)
    return jnp.where(rows == 0, high, jnp.where(rows == 1, full - high, 0.0)).astype(BF)


def single(row):
    rows = lax.broadcasted_iota(jnp.int32, (8, B), 0)
    return jnp.where(rows == 0, jnp.broadcast_to(row, (8, B)), 0.0).astype(BF)


def joined(product):
    return product[0:1] + product[1:2]


def params():
    return pltpu.CompilerParams(
        dimension_semantics=("arbitrary",), vmem_limit_bytes=VMEM_LIMIT
    )


def whole(shape):
    return pl.BlockSpec(shape, lambda i, *_: (0,) * len(shape))


def start_kernel(rhs, inv, out, out_low):
    for j in range(rhs.shape[0]):
        row = OMEGA * joined(dot(split(rhs[j : j + 1]), inv[j], NT))
        out[j : j + 1] = row
    out_low[...] = out[...].astype(BF)


def first_sweep(rhs, inv, group=32):
    rows = rhs.shape[0]
    return pl.pallas_call(
        start_kernel,
        out_shape=(
            jax.ShapeDtypeStruct((rows, B), F32),
            jax.ShapeDtypeStruct((rows, B), BF),
        ),
        grid=(rows // group,),
        in_specs=[
            pl.BlockSpec((group, B), lambda i: (i, 0)),
            pl.BlockSpec((group, B, B), lambda i: (i, 0, 0)),
        ],
        out_specs=(
            pl.BlockSpec((group, B), lambda i: (i, 0)),
            pl.BlockSpec((group, B), lambda i: (i, 0)),
        ),
        compiler_params=params(),
        name="first_sweep",
    )(rhs, inv)


def defect_rows(i, group, slots, rows, rhs, x_group, table, low, high, diag, pair, far, tab, side, held):
    @pl.when(i == 0)
    def _():
        tab[...] = table[...].astype(F32)
        side[0:rows] = low[...].astype(F32)
        side[rows : 2 * rows] = high[...].astype(F32)

    for j in range(group):
        r = i * group + j
        mate = tab[pl.ds(slots[r], 1)]
        first = tab[pl.ds(slots[rows + r], 1)]
        second = side[pl.ds(slots[2 * rows + r], 1)]
        total = dot(split(x_group[j : j + 1]), diag[j], NT)
        total += dot(single(mate), pair[j], NT)
        total += dot(single(first), far[j, 0], NT)
        total += dot(single(second), far[j, 1], NT)
        held[j : j + 1] = rhs[j : j + 1] - joined(total)


def sweep_kernel(group, rows, slots, rhs, x_group, table, low, high, diag, pair, far, inv, out, out_low, tab, side, held):
    i = pl.program_id(0)
    defect_rows(i, group, slots, rows, rhs, x_group, table, low, high, diag, pair, far, tab, side, held)
    for j in range(group):
        step = joined(dot(split(held[j : j + 1]), inv[j], NT))
        out[j : j + 1] = x_group[j : j + 1] + OMEGA * step
    out_low[...] = out[...].astype(BF)


def residual_kernel(group, rows, slots, sends, rhs, x_group, table, low, high, diag, pair, far, prol, even, packed, tab, side, held, mail):
    i = pl.program_id(0)
    defect_rows(i, group, slots, rows, rhs, x_group, table, low, high, diag, pair, far, tab, side, held)

    @pl.when(i == 0)
    def _():
        mail[...] = jnp.zeros_like(mail)

    for j in range(group):
        value = joined(dot(split(held[j : j + 1]), prol[j], NN))
        if j % 2 == 0:
            even[j // 2 : j // 2 + 1] = value
        else:
            mail[pl.ds(sends[i * (group // 2) + j // 2], 1)] = value

    @pl.when(i == pl.num_programs(0) - 1)
    def _():
        packed[...] = mail[...].astype(BF)


def apply_specs(rows, group):
    row = pl.BlockSpec((group, B), lambda i, *_: (i, 0))
    block = pl.BlockSpec((group, B, B), lambda i, *_: (i, 0, 0))
    return [
        row,
        row,
        whole((16 * rows, B)),
        whole((rows, B)),
        whole((rows, B)),
        block,
        block,
        pl.BlockSpec((group, 2, B, B), lambda i, *_: (i, 0, 0, 0)),
        block,
    ]


def apply_scratch(rows, group):
    return [
        pltpu.VMEM((16 * rows, B), F32),
        pltpu.VMEM((2 * rows, B), F32),
        pltpu.VMEM((group, B), F32),
    ]


def second_sweep(slots, rhs, x, table, low, high, diag, pair, far, inv, group=16):
    rows = rhs.shape[0]
    row = pl.BlockSpec((group, B), lambda i, *_: (i, 0))
    return pl.pallas_call(
        functools.partial(sweep_kernel, group, rows),
        out_shape=(
            jax.ShapeDtypeStruct((rows, B), F32),
            jax.ShapeDtypeStruct((rows, B), BF),
        ),
        grid_spec=pltpu.PrefetchScalarGridSpec(
            num_scalar_prefetch=1,
            grid=(rows // group,),
            in_specs=apply_specs(rows, group),
            out_specs=(row, row),
            scratch_shapes=apply_scratch(rows, group),
        ),
        compiler_params=params(),
        name="second_sweep",
    )(slots, rhs, x, table, low, high, diag, pair, far, inv)


def residual_pieces(slots, sends, rhs, x, table, low, high, diag, pair, far, prol, group=16):
    rows = rhs.shape[0]
    return pl.pallas_call(
        functools.partial(residual_kernel, group, rows),
        out_shape=(
            jax.ShapeDtypeStruct((rows // 2, B), F32),
            jax.ShapeDtypeStruct((rows, B), BF),
        ),
        grid_spec=pltpu.PrefetchScalarGridSpec(
            num_scalar_prefetch=2,
            grid=(rows // group,),
            in_specs=apply_specs(rows, group),
            out_specs=(
                pl.BlockSpec((group // 2, B), lambda i, *_: (i, 0)),
                whole((rows, B)),
            ),
            scratch_shapes=apply_scratch(rows, group) + [pltpu.VMEM((rows, B), F32)],
        ),
        compiler_params=params(),
        name="residual_pieces",
    )(slots, sends, rhs, x, table, low, high, diag, pair, far, prol)


def odd_kernel(group, ranks, places, starts, prol, diag, pair, *rest):
    outs, (both, inner, buf, sem) = rest[:-4], rest[-4:]
    i = pl.program_id(0)
    for j in range(group):
        right = jnp.concatenate([diag[j, 0], pair[j, 0]], axis=1)
        both[j] = dot(prol[j, 0], right, TN).astype(BF)
    for j in range(group):
        inner[j] = dot(both[j, :, :B], prol[j, 0], NN).astype(BF)
    for j in range(group):
        place = places[i * group + j]
        buf[place, 0] = prol[j, 0]
        buf[place, 1] = both[j, :, B:]
        buf[place, 2] = inner[j]

    def copy(k):
        return pltpu.make_async_copy(
            buf.at[pl.ds(starts[k], ranks)], outs[k - 1], sem.at[k]
        )

    @pl.when(i == pl.num_programs(0) - 1)
    def _():
        for step in ("start", "wait"):
            for k in range(1, len(outs) + 1):

                @pl.when(starts[k] >= 0)
                def _():
                    getattr(copy(k), step)()


def odd_blocks(places, starts, ranks, prol, diag, pair, group=16):
    half = prol.shape[0] // 2
    parts = starts.shape[0] - 1
    odd = pl.BlockSpec((group, 1, B, B), lambda i, *_: (i, 1, 0, 0))
    return pl.pallas_call(
        functools.partial(odd_kernel, group, ranks),
        out_shape=(jax.ShapeDtypeStruct((ranks, 3, B, B), BF),) * parts,
        grid_spec=pltpu.PrefetchScalarGridSpec(
            num_scalar_prefetch=2,
            grid=(half // group,),
            in_specs=[odd, odd, odd],
            out_specs=(pl.BlockSpec(memory_space=pl.ANY),) * parts,
            scratch_shapes=[
                pltpu.VMEM((group, B, 2 * B), BF),
                pltpu.VMEM((group, B, B), BF),
                pltpu.VMEM((half, 3, B, B), BF),
                pltpu.SemaphoreType.DMA((parts + 1,)),
            ],
        ),
        compiler_params=params(),
        name="odd_blocks",
    )(places, starts, *[a.reshape(half, 2, B, B) for a in (prol, diag, pair)])


def even_kernel(prol, diag, pair, out):
    for j in range(prol.shape[0]):
        both = dot(prol[j, 0], jnp.concatenate([diag[j, 0], pair[j, 0]], axis=1), TN)
        out[j] = both.astype(BF)


def even_blocks(prol, diag, pair, group=16):
    half = prol.shape[0] // 2
    even = pl.BlockSpec((group, 1, B, B), lambda i, *_: (i, 0, 0, 0))
    return pl.pallas_call(
        even_kernel,
        out_shape=jax.ShapeDtypeStruct((half, B, 2 * B), BF),
        grid=(half // group,),
        in_specs=[even, even, even],
        out_specs=pl.BlockSpec((group, B, 2 * B), lambda i: (i, 0, 0)),
        compiler_params=params(),
        name="even_blocks",
    )(*[a.reshape(half, 2, B, B) for a in (prol, diag, pair)])


def coarse_kernel(group, ranks, recvs, places, starts, mail, even, own, prol, *rest):
    parts = rest[:-9]
    blocks, restricted, packed, lift, buf, sem, letters, reply, held = rest[-9:]
    i = pl.program_id(0)

    def copy(k):
        return pltpu.make_async_copy(
            parts[k - 1], buf.at[pl.ds(starts[k], ranks)], sem.at[k]
        )

    @pl.when(i == 0)
    def _():
        for step in ("start", "wait"):
            for k in range(1, len(parts) + 1):

                @pl.when(starts[k] >= 0)
                def _():
                    getattr(copy(k), step)()

        letters[...] = mail[...].astype(F32)
        reply[...] = jnp.zeros_like(reply)

    for j in range(group):
        place = places[i * group + j]
        p = prol[j, 0]
        left = jnp.concatenate([own[j, :, B:], buf[place, 1]], axis=1)
        right = jnp.concatenate([buf[place, 0], p], axis=0)
        total = dot(own[j, :, :B], p, NN) + dot(left, right, NN)
        blocks[j] = (total + buf[place, 2].astype(F32)).astype(BF)
    for j in range(group):
        slot = recvs[i * group + j]
        restricted[j : j + 1] = even[j : j + 1] + letters[pl.ds(slot, 1)]
    for j in range(group):
        r = restricted[j : j + 1]
        c = THETA * r
        held[j : j + 1] = c + THETA * (r - joined(dot(split(c), blocks[j], NT)))
    for j in range(group):
        lift[j : j + 1] = joined(dot(split(held[j : j + 1]), prol[j, 0], NT))
    for j in range(group):
        reply[pl.ds(recvs[i * group + j], 1)] = held[j : j + 1]

    @pl.when(i == pl.num_programs(0) - 1)
    def _():
        packed[...] = reply[...].astype(BF)


def coarse(recvs, places, starts, ranks, parts, mail, even, own, prol, group=16):
    half = even.shape[0]
    row = pl.BlockSpec((group, B), lambda i, *_: (i, 0))
    return pl.pallas_call(
        functools.partial(coarse_kernel, group, ranks),
        out_shape=(
            jax.ShapeDtypeStruct((half, B, B), BF),
            jax.ShapeDtypeStruct((half, B), F32),
            jax.ShapeDtypeStruct((2 * half, B), BF),
            jax.ShapeDtypeStruct((half, B), F32),
        ),
        grid_spec=pltpu.PrefetchScalarGridSpec(
            num_scalar_prefetch=3,
            grid=(half // group,),
            in_specs=[
                whole((2 * half, B)),
                row,
                pl.BlockSpec((group, B, 2 * B), lambda i, *_: (i, 0, 0)),
                pl.BlockSpec((group, 1, B, B), lambda i, *_: (i, 0, 0, 0)),
            ]
            + [pl.BlockSpec(memory_space=pl.ANY)] * len(parts),
            out_specs=(
                pl.BlockSpec((group, B, B), lambda i, *_: (i, 0, 0)),
                row,
                whole((2 * half, B)),
                row,
            ),
            scratch_shapes=[
                pltpu.VMEM((half, 3, B, B), BF),
                pltpu.SemaphoreType.DMA((len(parts) + 1,)),
                pltpu.VMEM((2 * half, B), F32),
                pltpu.VMEM((2 * half, B), F32),
                pltpu.VMEM((group, B), F32),
            ],
        ),
        compiler_params=params(),
        name="coarse",
    )(recvs, places, starts, mail, even, own, prol.reshape(half, 2, B, B), *parts)


def finish_kernel(group, sends, mail, lift, x, prol, out, letters):
    i = pl.program_id(0)

    @pl.when(i == 0)
    def _():
        letters[...] = mail[...].astype(F32)

    for j in range(group):
        e = 2 * j
        out[e : e + 1] = x[e : e + 1] + lift[j : j + 1]
        c = letters[pl.ds(sends[i * group + j], 1)]
        out[e + 1 : e + 2] = x[e + 1 : e + 2] + joined(dot(single(c), prol[j, 0], NT))


def finish(sends, mail, lift, x, prol, group=32):
    half = lift.shape[0]
    return pl.pallas_call(
        functools.partial(finish_kernel, group),
        out_shape=jax.ShapeDtypeStruct((2 * half, B), F32),
        grid_spec=pltpu.PrefetchScalarGridSpec(
            num_scalar_prefetch=1,
            grid=(half // group,),
            in_specs=[
                whole((2 * half, B)),
                pl.BlockSpec((group, B), lambda i, *_: (i, 0)),
                pl.BlockSpec((2 * group, B), lambda i, *_: (i, 0)),
                pl.BlockSpec((group, 1, B, B), lambda i, *_: (i, 1, 0, 0)),
            ],
            out_specs=pl.BlockSpec((2 * group, B), lambda i, *_: (i, 0)),
            scratch_shapes=[pltpu.VMEM((2 * half, B), F32)],
        ),
        compiler_params=params(),
        name="finish",
    )(sends, mail, lift, x, prol.reshape(half, 2, B, B))


def along(side, dx, dy):
    return [
        (x * side + y, (x + dx) % side * side + (y + dy) % side)
        for x in range(side)
        for y in range(side)
    ]


def gather_line(block):
    line = lax.axis_size("rx")
    return exchange(jnp.broadcast_to(block, (line,) + block.shape)).reshape(-1, B)


def neighbours(block):
    count = lax.axis_size("ry")
    forward = [(i, (i + 1) % count) for i in range(count)]
    backward = [(target, source) for source, target in forward]
    return lax.ppermute(block, "ry", forward), lax.ppermute(block, "ry", backward)


def exchange(packed):
    line = lax.axis_size("rx")
    shape = packed.shape
    out = lax.all_to_all(
        packed.reshape((line, -1) + shape[1:]), "rx", split_axis=0, concat_axis=0, tiled=True
    )
    return out.reshape(shape)


def body(rhs, a_diag, a_pair, a_far, approx_inv, prolong, col_index, partner, odd_owner):
    rows = rhs.shape[0]
    half = rows // 2
    line_size = lax.axis_size("rx")
    side_size = lax.axis_size("ry")
    line_pos = lax.axis_index("rx")
    side_pos = lax.axis_index("ry")
    grid_side = 4
    capacity = half // (line_size // 2)
    mate = jnp.stack([partner, 2 * odd_owner], axis=1).reshape(rows)

    def line_slot(global_row):
        return global_row // rows // side_size * rows + global_row % rows

    side_dev = col_index[:, 1] // rows
    below = side_dev % side_size == (side_pos - 1) % side_size
    side_slot = jnp.where(below, 0, rows) + col_index[:, 1] % rows
    slots = jnp.concatenate([line_slot(mate), line_slot(col_index[:, 0]), side_slot])

    item_ids = jnp.arange(half, dtype=jnp.int32)
    def offset_of(line, ahead):
        dx = ahead * (line // grid_side - line_pos // grid_side) % grid_side
        dy = ahead * (line - line_pos) % grid_side
        return dx * grid_side + dy

    def places_of(offset, rank):
        slot = offset * capacity + rank
        offsets = jnp.arange(line_size, dtype=jnp.int32)[:, None]
        places = jnp.sum(slot[None, :] < slot[:, None], axis=1, dtype=jnp.int32)
        starts = jnp.sum(offset[None, :] < offsets, axis=1, dtype=jnp.int32)
        used = jnp.any(offset[None, :] == offsets, axis=1)
        return places, jnp.where(used, starts, -1)

    target_line = odd_owner // half // side_size
    same_target = target_line[:, None] == target_line[None, :]
    earlier = odd_owner[None, :] < odd_owner[:, None]
    send_rank = jnp.sum(same_target & earlier, axis=1, dtype=jnp.int32)
    sends = target_line * capacity + send_rank
    send_places, send_starts = places_of(offset_of(target_line, 1), send_rank)
    source_line = partner // rows // side_size
    same_source = source_line[:, None] == source_line[None, :]
    before = item_ids[None, :] < item_ids[:, None]
    recv_rank = jnp.sum(same_source & before, axis=1, dtype=jnp.int32)
    recvs = source_line * capacity + recv_rank
    recv_places, recv_starts = places_of(offset_of(source_line, -1), recv_rank)

    barrier = lax.optimization_barrier
    leaving = list(
        odd_blocks(send_places, send_starts, capacity, prolong, a_diag, a_pair)
    )
    arrived = [None] * len(leaving)

    def leave(first, last, gate):
        picked = [dx * grid_side + dy - 1 for dx, dy in ORDER[first:last]]
        waits = [dx * grid_side + dy - 1 for dx, dy in ORDER[max(first - WINDOW, 0) : max(last - WINDOW, 0)]]
        ins, old, gate = barrier(([leaving[k] for k in picked], [arrived[k] for k in waits], gate))
        for k, part in zip(waits, old):
            arrived[k] = part
        for k, part in zip(picked, ins):
            dx, dy = divmod(k + 1, grid_side)
            arrived[k] = lax.ppermute(part, "rx", along(grid_side, dx, dy))
        return gate

    rhs = leave(0, 4, rhs)
    x, x_low = first_sweep(rhs, approx_inv)
    low, high = neighbours(x_low)
    table = gather_line(x_low)
    table = leave(4, 8, table)
    x, x_low = second_sweep(
        slots, rhs, x, table, low, high, a_diag, a_pair, a_far, approx_inv
    )
    low, high = neighbours(x_low)
    table = gather_line(x_low)
    table = leave(8, 12, table)
    own = even_blocks(prolong, a_diag, a_pair)
    even, mail = residual_pieces(
        slots, sends, rhs, x, table, low, high, a_diag, a_pair, a_far, prolong
    )
    mail = leave(12, 15, mail)
    mail = exchange(mail)
    blocks, restricted, reply, lift = coarse(
        recvs, recv_places, recv_starts, capacity, arrived, mail, even, own, prolong
    )
    fine = finish(sends, exchange(reply), lift, x, prolong)
    return fine, blocks, restricted


def solution(mesh):
    rows = P(("rx", "ry"))
    return jax.shard_map(
        body,
        mesh=mesh,
        in_specs=(rows,) * 9,
        out_specs=(rows,) * 3,
        check_vma=False,
    )
```

```python
import functools

import jax
import jax.numpy as jnp
from jax import lax
from jax.experimental import pallas as pl
from jax.experimental.pallas import tpu as pltpu
from jax.sharding import PartitionSpec as P

OMEGA = 0.7
THETA = 0.08
ORDER = (
    *((1, 1), (3, 3), (1, 3), (3, 1)),
    *((2, 1), (2, 3), (0, 1), (0, 3)),
    *((1, 2), (3, 2), (1, 0), (3, 0)),
    *((2, 2), (2, 0), (0, 2)),
)
WINDOW = 4
B = 128
VMEM_LIMIT = 48 * 1024 * 1024
BF = jnp.bfloat16
F32 = jnp.float32

NT = (((1,), (1,)), ((), ()))
NN = (((1,), (0,)), ((), ()))
TN = (((0,), (0,)), ((), ()))


def dot(left, right, dims):
    return lax.dot_general(left, right, dims, preferred_element_type=F32)


def split(row):
    rows = lax.broadcasted_iota(jnp.int32, (8, B), 0)
    full = jnp.broadcast_to(row, (8, B))
    high = full.astype(BF).astype(F32)
    return jnp.where(rows == 0, high, jnp.where(rows == 1, full - high, 0.0)).astype(BF)


def single(row):
    rows = lax.broadcasted_iota(jnp.int32, (8, B), 0)
    return jnp.where(rows == 0, jnp.broadcast_to(row, (8, B)), 0.0).astype(BF)


def joined(product):
    return product[0:1] + product[1:2]


def params():
    return pltpu.CompilerParams(
        dimension_semantics=("arbitrary",), vmem_limit_bytes=VMEM_LIMIT
    )


def whole(shape):
    return pl.BlockSpec(shape, lambda i, *_: (0,) * len(shape))


def start_kernel(rhs, inv, out, out_low):
    for j in range(rhs.shape[0]):
        row = OMEGA * joined(dot(split(rhs[j : j + 1]), inv[j], NT))
        out[j : j + 1] = row
    out_low[...] = out[...].astype(BF)


def first_sweep(rhs, inv, group=32):
    rows = rhs.shape[0]
    return pl.pallas_call(
        start_kernel,
        out_shape=(
            jax.ShapeDtypeStruct((rows, B), F32),
            jax.ShapeDtypeStruct((rows, B), BF),
        ),
        grid=(rows // group,),
        in_specs=[
            pl.BlockSpec((group, B), lambda i: (i, 0)),
            pl.BlockSpec((group, B, B), lambda i: (i, 0, 0)),
        ],
        out_specs=(
            pl.BlockSpec((group, B), lambda i: (i, 0)),
            pl.BlockSpec((group, B), lambda i: (i, 0)),
        ),
        compiler_params=params(),
        name="first_sweep",
    )(rhs, inv)


def defect_rows(i, group, slots, rows, rhs, x_group, table, low, high, diag, pair, far, tab, side, held):
    @pl.when(i == 0)
    def _():
        tab[...] = table[...].astype(F32)
        side[0:rows] = low[...].astype(F32)
        side[rows : 2 * rows] = high[...].astype(F32)

    for j in range(group):
        r = i * group + j
        mate = tab[pl.ds(slots[r], 1)]
        first = tab[pl.ds(slots[rows + r], 1)]
        second = side[pl.ds(slots[2 * rows + r], 1)]
        total = dot(split(x_group[j : j + 1]), diag[j], NT)
        total += dot(single(mate), pair[j], NT)
        total += dot(single(first), far[j, 0], NT)
        total += dot(single(second), far[j, 1], NT)
        held[j : j + 1] = rhs[j : j + 1] - joined(total)


def sweep_kernel(group, rows, slots, rhs, x_group, table, low, high, diag, pair, far, inv, out, out_low, tab, side, held):
    i = pl.program_id(0)
    defect_rows(i, group, slots, rows, rhs, x_group, table, low, high, diag, pair, far, tab, side, held)
    for j in range(group):
        step = joined(dot(split(held[j : j + 1]), inv[j], NT))
        out[j : j + 1] = x_group[j : j + 1] + OMEGA * step
    out_low[...] = out[...].astype(BF)


def residual_kernel(group, rows, slots, sends, rhs, x_group, table, low, high, diag, pair, far, prol, even, packed, tab, side, held, mail):
    i = pl.program_id(0)
    defect_rows(i, group, slots, rows, rhs, x_group, table, low, high, diag, pair, far, tab, side, held)

    @pl.when(i == 0)
    def _():
        mail[...] = jnp.zeros_like(mail)

    for j in range(group):
        value = joined(dot(split(held[j : j + 1]), prol[j], NN))
        if j % 2 == 0:
            even[j // 2 : j // 2 + 1] = value
        else:
            mail[pl.ds(sends[i * (group // 2) + j // 2], 1)] = value

    @pl.when(i == pl.num_programs(0) - 1)
    def _():
        packed[...] = mail[...].astype(BF)


def apply_specs(rows, group):
    row = pl.BlockSpec((group, B), lambda i, *_: (i, 0))
    block = pl.BlockSpec((group, B, B), lambda i, *_: (i, 0, 0))
    return [
        row,
        row,
        whole((16 * rows, B)),
        whole((rows, B)),
        whole((rows, B)),
        block,
        block,
        pl.BlockSpec((group, 2, B, B), lambda i, *_: (i, 0, 0, 0)),
        block,
    ]


def apply_scratch(rows, group):
    return [
        pltpu.VMEM((16 * rows, B), F32),
        pltpu.VMEM((2 * rows, B), F32),
        pltpu.VMEM((group, B), F32),
    ]


def second_sweep(slots, rhs, x, table, low, high, diag, pair, far, inv, group=16):
    rows = rhs.shape[0]
    row = pl.BlockSpec((group, B), lambda i, *_: (i, 0))
    return pl.pallas_call(
        functools.partial(sweep_kernel, group, rows),
        out_shape=(
            jax.ShapeDtypeStruct((rows, B), F32),
            jax.ShapeDtypeStruct((rows, B), BF),
        ),
        grid_spec=pltpu.PrefetchScalarGridSpec(
            num_scalar_prefetch=1,
            grid=(rows // group,),
            in_specs=apply_specs(rows, group),
            out_specs=(row, row),
            scratch_shapes=apply_scratch(rows, group),
        ),
        compiler_params=params(),
        name="second_sweep",
    )(slots, rhs, x, table, low, high, diag, pair, far, inv)


def residual_pieces(slots, sends, rhs, x, table, low, high, diag, pair, far, prol, group=16):
    rows = rhs.shape[0]
    return pl.pallas_call(
        functools.partial(residual_kernel, group, rows),
        out_shape=(
            jax.ShapeDtypeStruct((rows // 2, B), F32),
            jax.ShapeDtypeStruct((rows, B), BF),
        ),
        grid_spec=pltpu.PrefetchScalarGridSpec(
            num_scalar_prefetch=2,
            grid=(rows // group,),
            in_specs=apply_specs(rows, group),
            out_specs=(
                pl.BlockSpec((group // 2, B), lambda i, *_: (i, 0)),
                whole((rows, B)),
            ),
            scratch_shapes=apply_scratch(rows, group) + [pltpu.VMEM((rows, B), F32)],
        ),
        compiler_params=params(),
        name="residual_pieces",
    )(slots, sends, rhs, x, table, low, high, diag, pair, far, prol)


def odd_kernel(group, ranks, places, starts, prol, diag, pair, *rest):
    outs, (both, inner, buf, sem) = rest[:-4], rest[-4:]
    i = pl.program_id(0)
    for j in range(group):
        right = jnp.concatenate([diag[j, 0], pair[j, 0]], axis=1)
        both[j] = dot(prol[j, 0], right, TN).astype(BF)
    for j in range(group):
        inner[j] = dot(both[j, :, :B], prol[j, 0], NN).astype(BF)
    for j in range(group):
        place = places[i * group + j]
        buf[place, 0] = prol[j, 0]
        buf[place, 1] = both[j, :, B:]
        buf[place, 2] = inner[j]

    def copy(k):
        return pltpu.make_async_copy(
            buf.at[pl.ds(starts[k], ranks)], outs[k], sem.at[k]
        )

    @pl.when(i == pl.num_programs(0) - 1)
    def _():
        for step in ("start", "wait"):
            for k in range(len(outs)):

                @pl.when(starts[k] >= 0)
                def _():
                    getattr(copy(k), step)()


def odd_blocks(places, starts, ranks, prol, diag, pair, group=16):
    half = prol.shape[0] // 2
    parts = starts.shape[0]
    odd = pl.BlockSpec((group, 1, B, B), lambda i, *_: (i, 1, 0, 0))
    return pl.pallas_call(
        functools.partial(odd_kernel, group, ranks),
        out_shape=(jax.ShapeDtypeStruct((ranks, 3, B, B), BF),) * parts,
        grid_spec=pltpu.PrefetchScalarGridSpec(
            num_scalar_prefetch=2,
            grid=(half // group,),
            in_specs=[odd, odd, odd],
            out_specs=(pl.BlockSpec(memory_space=pl.ANY),) * parts,
            scratch_shapes=[
                pltpu.VMEM((group, B, 2 * B), BF),
                pltpu.VMEM((group, B, B), BF),
                pltpu.VMEM((half, 3, B, B), BF),
                pltpu.SemaphoreType.DMA((parts,)),
            ],
        ),
        compiler_params=params(),
        name="odd_blocks",
    )(places, starts, *[a.reshape(half, 2, B, B) for a in (prol, diag, pair)])


def even_kernel(group, places, prol, diag, pair, out, both):
    i = pl.program_id(0)
    for j in range(group):
        right = jnp.concatenate([diag[j, 0], pair[j, 0]], axis=1)
        both[j] = dot(prol[j, 0], right, TN).astype(BF)
    for j in range(group):
        place = places[i * group + j]
        out[place, :, : 2 * B] = both[j]
        out[place, :, 2 * B :] = prol[j, 0]


def even_blocks(places, prol, diag, pair, group=16):
    half = prol.shape[0] // 2
    even = pl.BlockSpec((group, 1, B, B), lambda i, *_: (i, 0, 0, 0))
    return pl.pallas_call(
        functools.partial(even_kernel, group),
        out_shape=jax.ShapeDtypeStruct((half, B, 3 * B), BF),
        grid_spec=pltpu.PrefetchScalarGridSpec(
            num_scalar_prefetch=1,
            grid=(half // group,),
            in_specs=[even, even, even],
            out_specs=whole((half, B, 3 * B)),
            scratch_shapes=[pltpu.VMEM((group, B, 2 * B), BF)],
        ),
        compiler_params=params(),
        name="even_blocks",
    )(places, *[a.reshape(half, 2, B, B) for a in (prol, diag, pair)])


def coarse_rows(i, first, ranks, items, recvs, even, own, buf, blk, sem, letters, blocks, restricted, reply, lift, held, last):
    def copy(at):
        return pltpu.make_async_copy(blk.at[at], blocks.at[items[first + at]], sem.at[at])

    base = i * ranks
    for j in range(ranks):
        p = own[j, :, 2 * B :]
        left = jnp.concatenate([own[j, :, B : 2 * B], buf[base + j, 1]], axis=1)
        right = jnp.concatenate([buf[base + j, 0], p], axis=0)
        total = dot(own[j, :, :B], p, NN) + dot(left, right, NN)
        blk[base + j] = (total + buf[base + j, 2].astype(F32)).astype(BF)
    for j in range(ranks):
        copy(base + j).start()
    for j in range(ranks):
        item = items[first + base + j]
        r = even[pl.ds(item, 1)] + letters[pl.ds(recvs[item], 1)]
        held[j : j + 1] = r
    for j in range(ranks):
        r = held[j : j + 1]
        c = THETA * r
        c = c + THETA * (r - joined(dot(split(c), blk[base + j], NT)))
        held[ranks + j : ranks + j + 1] = c
    for j in range(ranks):
        c = held[ranks + j : ranks + j + 1]
        held[2 * ranks + j : 2 * ranks + j + 1] = joined(dot(split(c), own[j, :, 2 * B :], NT))
    for j in range(ranks):
        item = items[first + base + j]
        restricted[pl.ds(item, 1)] = held[j : j + 1]
        reply[pl.ds(recvs[item], 1)] = held[ranks + j : ranks + j + 1]
        lift[pl.ds(item, 1)] = held[2 * ranks + j : 2 * ranks + j + 1]

    @pl.when(last)
    def _():
        for at in range(blk.shape[0]):
            copy(at).wait()


def early_kernel(ranks, early, items, recvs, starts, mail, even, own, *rest):
    parts = rest[:-11]
    blocks, rest_out, restricted, reply, lift, buf, blk, sem, part_sem, letters, held = rest[-11:]
    i = pl.program_id(0)

    def near(k):
        return pltpu.make_async_copy(
            parts[k], buf.at[pl.ds(starts[k], ranks)], part_sem.at[k]
        )

    later = pltpu.make_async_copy(
        buf.at[pl.ds(early, buf.shape[0] - early)], rest_out, part_sem.at[len(parts)]
    )

    @pl.when(i == 0)
    def _():
        for step in ("start", "wait"):
            for k in range(len(parts)):

                @pl.when(starts[k] >= 0)
                def _():
                    getattr(near(k), step)()

        later.start()
        letters[...] = mail[...].astype(F32)
        reply[...] = jnp.zeros_like(reply)
        restricted[...] = jnp.zeros_like(restricted)
        lift[...] = jnp.zeros_like(lift)

    last = i == pl.num_programs(0) - 1

    @pl.when(last)
    def _():
        later.wait()

    coarse_rows(i, 0, ranks, items, recvs, even, own, buf, blk, sem, letters, blocks, restricted, reply, lift, held, last)


def late_kernel(ranks, early, seen, items, recvs, starts, mail, even, own, before_r, before_y, before_l, blocks_in, rest_in, *rest):
    parts = rest[:-10]
    blocks, restricted, packed, lift, buf, blk, sem, part_sem, letters, held_all = rest[-10:]
    reply, held = held_all.at[pl.ds(0, letters.shape[0])], held_all.at[pl.ds(letters.shape[0], 4 * ranks)]
    i = pl.program_id(0)
    groups = buf.shape[0] // ranks

    def fresh(k):
        return pltpu.make_async_copy(
            parts[k - seen], buf.at[pl.ds(starts[k] - early, ranks)], part_sem.at[k]
        )

    def kept(k):
        at = pl.ds(starts[k] - early, ranks)
        return pltpu.make_async_copy(rest_in.at[at], buf.at[at], part_sem.at[k])

    @pl.when(i == 0)
    def _():
        for step in ("start", "wait"):
            for k in range(early // ranks, seen + len(parts)):

                @pl.when(starts[k] >= early)
                def _():
                    getattr(kept(k) if k < seen else fresh(k), step)()

        letters[...] = mail[...].astype(F32)
        reply[...] = before_y[...]
        restricted[...] = before_r[...]
        lift[...] = before_l[...]

    last = i == groups - 1
    coarse_rows(i, early, ranks, items, recvs, even, own, buf, blk, sem, letters, blocks, restricted, reply, lift, held, last)

    @pl.when(last)
    def _():
        packed[...] = reply[...].astype(BF)


def coarse_early(items, recvs, starts, ranks, early, parts, mail, even, own):
    half = even.shape[0]
    anywhere = pl.BlockSpec(memory_space=pl.ANY)
    return pl.pallas_call(
        functools.partial(early_kernel, ranks, early),
        out_shape=(
            jax.ShapeDtypeStruct((half, B, B), BF),
            jax.ShapeDtypeStruct((half - early, 3, B, B), BF),
            jax.ShapeDtypeStruct((half, B), F32),
            jax.ShapeDtypeStruct((2 * half, B), F32),
            jax.ShapeDtypeStruct((half, B), F32),
        ),
        grid_spec=pltpu.PrefetchScalarGridSpec(
            num_scalar_prefetch=3,
            grid=(early // ranks,),
            in_specs=[
                whole((2 * half, B)),
                whole((half, B)),
                pl.BlockSpec((ranks, B, 3 * B), lambda i, *_: (i, 0, 0)),
            ]
            + [anywhere] * len(parts),
            out_specs=(
                anywhere,
                anywhere,
                whole((half, B)),
                whole((2 * half, B)),
                whole((half, B)),
            ),
            scratch_shapes=[
                pltpu.VMEM((half, 3, B, B), BF),
                pltpu.VMEM((early, B, B), BF),
                pltpu.SemaphoreType.DMA((early,)),
                pltpu.SemaphoreType.DMA((len(parts) + 1,)),
                pltpu.VMEM((2 * half, B), F32),
                pltpu.VMEM((4 * ranks, B), F32),
            ],
        ),
        compiler_params=params(),
        name="coarse_early",
    )(items, recvs, starts, mail, even, own, *parts)


def coarse_late(items, recvs, starts, ranks, early, seen, parts, mail, even, own, restricted, reply, lift, blocks, kept):
    half = even.shape[0]
    late = half - early
    anywhere = pl.BlockSpec(memory_space=pl.ANY)
    return pl.pallas_call(
        functools.partial(late_kernel, ranks, early, seen),
        out_shape=(
            jax.ShapeDtypeStruct((half, B, B), BF),
            jax.ShapeDtypeStruct((half, B), F32),
            jax.ShapeDtypeStruct((2 * half, B), BF),
            jax.ShapeDtypeStruct((half, B), F32),
        ),
        grid_spec=pltpu.PrefetchScalarGridSpec(
            num_scalar_prefetch=3,
            grid=(late // ranks,),
            in_specs=[
                whole((2 * half, B)),
                whole((half, B)),
                pl.BlockSpec((ranks, B, 3 * B), lambda i, *_: (i + early // ranks, 0, 0)),
                whole((half, B)),
                whole((2 * half, B)),
                whole((half, B)),
                anywhere,
                anywhere,
            ]
            + [anywhere] * len(parts),
            out_specs=(anywhere, whole((half, B)), whole((2 * half, B)), whole((half, B))),
            scratch_shapes=[
                pltpu.VMEM((late, 3, B, B), BF),
                pltpu.VMEM((late, B, B), BF),
                pltpu.SemaphoreType.DMA((late,)),
                pltpu.SemaphoreType.DMA((seen + len(parts),)),
                pltpu.VMEM((2 * half, B), F32),
                pltpu.VMEM((2 * half + 4 * ranks, B), F32),
            ],
        ),
        input_output_aliases={9: 0},
        compiler_params=params(),
        name="coarse_late",
    )(items, recvs, starts, mail, even, own, restricted, reply, lift, blocks, kept, *parts)


def finish_kernel(group, sends, mail, lift, x, prol, out, letters):
    i = pl.program_id(0)

    @pl.when(i == 0)
    def _():
        letters[...] = mail[...].astype(F32)

    for j in range(group):
        e = 2 * j
        out[e : e + 1] = x[e : e + 1] + lift[j : j + 1]
        c = letters[pl.ds(sends[i * group + j], 1)]
        out[e + 1 : e + 2] = x[e + 1 : e + 2] + joined(dot(single(c), prol[j, 0], NT))


def finish(sends, mail, lift, x, prol, group=32):
    half = lift.shape[0]
    return pl.pallas_call(
        functools.partial(finish_kernel, group),
        out_shape=jax.ShapeDtypeStruct((2 * half, B), F32),
        grid_spec=pltpu.PrefetchScalarGridSpec(
            num_scalar_prefetch=1,
            grid=(half // group,),
            in_specs=[
                whole((2 * half, B)),
                pl.BlockSpec((group, B), lambda i, *_: (i, 0)),
                pl.BlockSpec((2 * group, B), lambda i, *_: (i, 0)),
                pl.BlockSpec((group, 1, B, B), lambda i, *_: (i, 1, 0, 0)),
            ],
            out_specs=pl.BlockSpec((2 * group, B), lambda i, *_: (i, 0)),
            scratch_shapes=[pltpu.VMEM((2 * half, B), F32)],
        ),
        compiler_params=params(),
        name="finish",
    )(sends, mail, lift, x, prol.reshape(half, 2, B, B))


def along(side, dx, dy):
    return [
        (x * side + y, (x + dx) % side * side + (y + dy) % side)
        for x in range(side)
        for y in range(side)
    ]


def gather_line(block):
    line = lax.axis_size("rx")
    copies = jnp.broadcast_to(block, (line,) + block.shape)
    gathered = lax.all_to_all(copies, "rx", split_axis=0, concat_axis=0, tiled=True)
    return gathered.reshape(-1, B)


def neighbours(block):
    count = lax.axis_size("ry")
    forward = [(i, (i + 1) % count) for i in range(count)]
    backward = [(target, source) for source, target in forward]
    return lax.ppermute(block, "ry", forward), lax.ppermute(block, "ry", backward)


def exchange(packed):
    line = lax.axis_size("rx")
    shape = packed.shape
    out = lax.all_to_all(
        packed.reshape((line, -1) + shape[1:]), "rx", split_axis=0, concat_axis=0, tiled=True
    )
    return out.reshape(shape)


def body(rhs, a_diag, a_pair, a_far, approx_inv, prolong, col_index, partner, odd_owner):
    rows = rhs.shape[0]
    half = rows // 2
    line_size = lax.axis_size("rx")
    side_size = lax.axis_size("ry")
    line_pos = lax.axis_index("rx")
    side_pos = lax.axis_index("ry")
    grid_side = 4
    capacity = half // (line_size // 2)
    mate = jnp.stack([partner, 2 * odd_owner], axis=1).reshape(rows)

    def line_slot(global_row):
        return global_row // rows // side_size * rows + global_row % rows

    side_dev = col_index[:, 1] // rows
    below = side_dev % side_size == (side_pos - 1) % side_size
    side_slot = jnp.where(below, 0, rows) + col_index[:, 1] % rows
    slots = jnp.concatenate([line_slot(mate), line_slot(col_index[:, 0]), side_slot])

    item_ids = jnp.arange(half, dtype=jnp.int32)
    codes = jnp.array([dx * grid_side + dy for dx, dy in ORDER], jnp.int32)[:, None]
    turns = jnp.arange(len(ORDER), dtype=jnp.int32)[:, None]

    def turn_of(line, ahead):
        dx = ahead * (line // grid_side - line_pos // grid_side) % grid_side
        dy = ahead * (line - line_pos) % grid_side
        hits = (dx * grid_side + dy)[None, :] == codes
        return jnp.sum(jnp.where(hits, turns, 0), axis=0, dtype=jnp.int32)

    def places_of(turn, rank):
        slot = turn * capacity + rank
        places = jnp.sum(slot[None, :] < slot[:, None], axis=1, dtype=jnp.int32)
        starts = jnp.sum(turn[None, :] < turns, axis=1, dtype=jnp.int32)
        used = jnp.any(turn[None, :] == turns, axis=1)
        return places, jnp.where(used, starts, -1)

    target_line = odd_owner // half // side_size
    same_target = target_line[:, None] == target_line[None, :]
    earlier = odd_owner[None, :] < odd_owner[:, None]
    send_rank = jnp.sum(same_target & earlier, axis=1, dtype=jnp.int32)
    sends = target_line * capacity + send_rank
    send_places, send_starts = places_of(turn_of(target_line, 1), send_rank)
    source_line = partner // rows // side_size
    same_source = source_line[:, None] == source_line[None, :]
    before = item_ids[None, :] < item_ids[:, None]
    recv_rank = jnp.sum(same_source & before, axis=1, dtype=jnp.int32)
    recvs = source_line * capacity + recv_rank
    recv_places, recv_starts = places_of(turn_of(source_line, -1), recv_rank)

    hits = recv_places[None, :] == item_ids[:, None]
    items = jnp.sum(jnp.where(hits, item_ids[None, :], 0), axis=1, dtype=jnp.int32)

    leaving = odd_blocks(send_places, send_starts, capacity, prolong, a_diag, a_pair)
    arrived = []

    def leave(first, last, gate):
        wait = max(first - WINDOW, 0)
        ins, old, gate = lax.optimization_barrier((leaving[first:last], arrived[wait:], gate))
        arrived[wait:] = old
        for part, (dx, dy) in zip(ins, ORDER[first:last]):
            arrived.append(lax.ppermute(part, "rx", along(grid_side, dx, dy)))
        return gate

    rhs = leave(0, 4, rhs)
    x, x_low = first_sweep(rhs, approx_inv)
    low, high = neighbours(x_low)
    table = gather_line(x_low)
    table = leave(4, 8, table)
    x, x_low = second_sweep(
        slots, rhs, x, table, low, high, a_diag, a_pair, a_far, approx_inv
    )
    low, high = neighbours(x_low)
    table = gather_line(x_low)
    table = leave(8, 12, table)
    own = even_blocks(recv_places, prolong, a_diag, a_pair)
    even, mail = residual_pieces(
        slots, sends, rhs, x, table, low, high, a_diag, a_pair, a_far, prolong
    )
    mail = exchange(mail)
    mail = leave(12, 15, mail)
    late = 3 * capacity
    early = half - late
    blocks, kept, restricted, reply, lift = coarse_early(
        items, recvs, recv_starts, capacity, early, arrived[:12], mail, even, own
    )
    blocks, restricted, reply, lift = coarse_late(
        items, recvs, recv_starts, capacity, early, 12, arrived[12:], mail, even, own, restricted, reply, lift, blocks, kept
    )
    fine = finish(sends, exchange(reply), lift, x, prolong)
    return fine, blocks, restricted


def solution(mesh):
    rows = P(("rx", "ry"))
    return jax.shard_map(
        body,
        mesh=mesh,
        in_specs=(rows,) * 9,
        out_specs=(rows,) * 3,
        check_vma=False,
    )
```

```python
import functools

import jax
import jax.numpy as jnp
from jax import lax
from jax.experimental import pallas as pl
from jax.experimental.pallas import tpu as pltpu
from jax.sharding import PartitionSpec as P

OMEGA = 0.7
THETA = 0.08
ORDER = (
    *((1, 1), (3, 3), (1, 3), (3, 1)),
    *((2, 1), (2, 3), (0, 1), (0, 3)),
    *((1, 2), (3, 2), (1, 0), (3, 0)),
    *((2, 2), (2, 0), (0, 2)),
)
WINDOW = 4
B = 128
VMEM_LIMIT = 48 * 1024 * 1024
BF = jnp.bfloat16
F32 = jnp.float32

NT = (((1,), (1,)), ((), ()))
NN = (((1,), (0,)), ((), ()))
TN = (((0,), (0,)), ((), ()))


def dot(left, right, dims):
    return lax.dot_general(left, right, dims, preferred_element_type=F32)


def split(row):
    rows = lax.broadcasted_iota(jnp.int32, (8, B), 0)
    full = jnp.broadcast_to(row, (8, B))
    high = full.astype(BF).astype(F32)
    return jnp.where(rows == 0, high, jnp.where(rows == 1, full - high, 0.0)).astype(BF)


def single(row):
    rows = lax.broadcasted_iota(jnp.int32, (8, B), 0)
    return jnp.where(rows == 0, jnp.broadcast_to(row, (8, B)), 0.0).astype(BF)


def joined(product):
    return product[0:1] + product[1:2]


def params():
    return pltpu.CompilerParams(
        dimension_semantics=("arbitrary",), vmem_limit_bytes=VMEM_LIMIT
    )


def whole(shape):
    return pl.BlockSpec(shape, lambda i, *_: (0,) * len(shape))


def start_kernel(rhs, inv, out, out_low):
    for j in range(rhs.shape[0]):
        row = OMEGA * joined(dot(split(rhs[j : j + 1]), inv[j], NT))
        out[j : j + 1] = row
    out_low[...] = out[...].astype(BF)


def first_sweep(rhs, inv, group=32):
    rows = rhs.shape[0]
    return pl.pallas_call(
        start_kernel,
        out_shape=(
            jax.ShapeDtypeStruct((rows, B), F32),
            jax.ShapeDtypeStruct((rows, B), BF),
        ),
        grid=(rows // group,),
        in_specs=[
            pl.BlockSpec((group, B), lambda i: (i, 0)),
            pl.BlockSpec((group, B, B), lambda i: (i, 0, 0)),
        ],
        out_specs=(
            pl.BlockSpec((group, B), lambda i: (i, 0)),
            pl.BlockSpec((group, B), lambda i: (i, 0)),
        ),
        compiler_params=params(),
        name="first_sweep",
    )(rhs, inv)


def defect_rows(i, group, slots, rows, rhs, x_group, table, low, high, diag, pair, far, tab, side, held):
    @pl.when(i == 0)
    def _():
        tab[...] = table[...].astype(F32)
        side[0:rows] = low[...].astype(F32)
        side[rows : 2 * rows] = high[...].astype(F32)

    for j in range(group):
        r = i * group + j
        mate = tab[pl.ds(slots[r], 1)]
        first = tab[pl.ds(slots[rows + r], 1)]
        second = side[pl.ds(slots[2 * rows + r], 1)]
        total = dot(split(x_group[j : j + 1]), diag[j], NT)
        total += dot(single(mate), pair[j], NT)
        total += dot(single(first), far[j, 0], NT)
        total += dot(single(second), far[j, 1], NT)
        held[j : j + 1] = rhs[j : j + 1] - joined(total)


def sweep_kernel(group, rows, slots, rhs, x_group, table, low, high, diag, pair, far, inv, out, out_low, tab, side, held):
    i = pl.program_id(0)
    defect_rows(i, group, slots, rows, rhs, x_group, table, low, high, diag, pair, far, tab, side, held)
    for j in range(group):
        step = joined(dot(split(held[j : j + 1]), inv[j], NT))
        out[j : j + 1] = x_group[j : j + 1] + OMEGA * step
    out_low[...] = out[...].astype(BF)


def residual_kernel(group, rows, slots, sends, rhs, x_group, table, low, high, diag, pair, far, prol, even, packed, tab, side, held, mail):
    i = pl.program_id(0)
    defect_rows(i, group, slots, rows, rhs, x_group, table, low, high, diag, pair, far, tab, side, held)

    @pl.when(i == 0)
    def _():
        mail[...] = jnp.zeros_like(mail)

    for j in range(group):
        value = joined(dot(split(held[j : j + 1]), prol[j], NN))
        if j % 2 == 0:
            even[j // 2 : j // 2 + 1] = value
        else:
            mail[pl.ds(sends[i * (group // 2) + j // 2], 1)] = value

    @pl.when(i == pl.num_programs(0) - 1)
    def _():
        packed[...] = mail[...].astype(BF)


def apply_specs(rows, group):
    row = pl.BlockSpec((group, B), lambda i, *_: (i, 0))
    block = pl.BlockSpec((group, B, B), lambda i, *_: (i, 0, 0))
    return [
        row,
        row,
        whole((16 * rows, B)),
        whole((rows, B)),
        whole((rows, B)),
        block,
        block,
        pl.BlockSpec((group, 2, B, B), lambda i, *_: (i, 0, 0, 0)),
        block,
    ]


def apply_scratch(rows, group):
    return [
        pltpu.VMEM((16 * rows, B), F32),
        pltpu.VMEM((2 * rows, B), F32),
        pltpu.VMEM((group, B), F32),
    ]


def second_sweep(slots, rhs, x, table, low, high, diag, pair, far, inv, group=16):
    rows = rhs.shape[0]
    row = pl.BlockSpec((group, B), lambda i, *_: (i, 0))
    return pl.pallas_call(
        functools.partial(sweep_kernel, group, rows),
        out_shape=(
            jax.ShapeDtypeStruct((rows, B), F32),
            jax.ShapeDtypeStruct((rows, B), BF),
        ),
        grid_spec=pltpu.PrefetchScalarGridSpec(
            num_scalar_prefetch=1,
            grid=(rows // group,),
            in_specs=apply_specs(rows, group),
            out_specs=(row, row),
            scratch_shapes=apply_scratch(rows, group),
        ),
        compiler_params=params(),
        name="second_sweep",
    )(slots, rhs, x, table, low, high, diag, pair, far, inv)


def residual_pieces(slots, sends, rhs, x, table, low, high, diag, pair, far, prol, group=16):
    rows = rhs.shape[0]
    return pl.pallas_call(
        functools.partial(residual_kernel, group, rows),
        out_shape=(
            jax.ShapeDtypeStruct((rows // 2, B), F32),
            jax.ShapeDtypeStruct((rows, B), BF),
        ),
        grid_spec=pltpu.PrefetchScalarGridSpec(
            num_scalar_prefetch=2,
            grid=(rows // group,),
            in_specs=apply_specs(rows, group),
            out_specs=(
                pl.BlockSpec((group // 2, B), lambda i, *_: (i, 0)),
                whole((rows, B)),
            ),
            scratch_shapes=apply_scratch(rows, group) + [pltpu.VMEM((rows, B), F32)],
        ),
        compiler_params=params(),
        name="residual_pieces",
    )(slots, sends, rhs, x, table, low, high, diag, pair, far, prol)


def odd_kernel(group, ranks, places, starts, prol, diag, pair, *rest):
    outs, (both, inner, buf, sem) = rest[:-4], rest[-4:]
    i = pl.program_id(0)
    for j in range(group):
        right = jnp.concatenate([diag[j, 0], pair[j, 0]], axis=1)
        both[j] = dot(prol[j, 0], right, TN).astype(BF)
    for j in range(group):
        inner[j] = dot(both[j, :, :B], prol[j, 0], NN).astype(BF)
    for j in range(group):
        place = places[i * group + j]
        buf[place, 0] = prol[j, 0]
        buf[place, 1] = both[j, :, B:]
        buf[place, 2] = inner[j]

    def copy(k):
        return pltpu.make_async_copy(
            buf.at[pl.ds(starts[k], ranks)], outs[k], sem.at[k]
        )

    @pl.when(i == pl.num_programs(0) - 1)
    def _():
        for step in ("start", "wait"):
            for k in range(len(outs)):

                @pl.when(starts[k] >= 0)
                def _():
                    getattr(copy(k), step)()


def odd_blocks(places, starts, ranks, prol, diag, pair, group=16):
    half = prol.shape[0] // 2
    parts = starts.shape[0]
    odd = pl.BlockSpec((group, 1, B, B), lambda i, *_: (i, 1, 0, 0))
    return pl.pallas_call(
        functools.partial(odd_kernel, group, ranks),
        out_shape=(jax.ShapeDtypeStruct((ranks, 3, B, B), BF),) * parts,
        grid_spec=pltpu.PrefetchScalarGridSpec(
            num_scalar_prefetch=2,
            grid=(half // group,),
            in_specs=[odd, odd, odd],
            out_specs=(pl.BlockSpec(memory_space=pl.ANY),) * parts,
            scratch_shapes=[
                pltpu.VMEM((group, B, 2 * B), BF),
                pltpu.VMEM((group, B, B), BF),
                pltpu.VMEM((half, 3, B, B), BF),
                pltpu.SemaphoreType.DMA((parts,)),
            ],
        ),
        compiler_params=params(),
        name="odd_blocks",
    )(places, starts, *[a.reshape(half, 2, B, B) for a in (prol, diag, pair)])


def even_kernel(group, places, prol, diag, pair, out, both):
    i = pl.program_id(0)
    for j in range(group):
        right = jnp.concatenate([diag[j, 0], pair[j, 0]], axis=1)
        both[j] = dot(prol[j, 0], right, TN).astype(BF)
    for j in range(group):
        place = places[i * group + j]
        out[place, :, : 2 * B] = both[j]
        out[place, :, 2 * B :] = prol[j, 0]


def even_blocks(places, prol, diag, pair, group=16):
    half = prol.shape[0] // 2
    even = pl.BlockSpec((group, 1, B, B), lambda i, *_: (i, 0, 0, 0))
    return pl.pallas_call(
        functools.partial(even_kernel, group),
        out_shape=jax.ShapeDtypeStruct((half, B, 3 * B), BF),
        grid_spec=pltpu.PrefetchScalarGridSpec(
            num_scalar_prefetch=1,
            grid=(half // group,),
            in_specs=[even, even, even],
            out_specs=whole((half, B, 3 * B)),
            scratch_shapes=[pltpu.VMEM((group, B, 2 * B), BF)],
        ),
        compiler_params=params(),
        name="even_blocks",
    )(places, *[a.reshape(half, 2, B, B) for a in (prol, diag, pair)])


def coarse_rows(i, first, ranks, items, recvs, even, own, buf, blk, sem, letters, blocks, restricted, reply, lift, held, last):
    def copy(at):
        return pltpu.make_async_copy(blk.at[at], blocks.at[items[first + at]], sem.at[at])

    base = i * ranks
    for j in range(ranks):
        p = own[j, :, 2 * B :]
        left = jnp.concatenate([own[j, :, B : 2 * B], buf[base + j, 1]], axis=1)
        right = jnp.concatenate([buf[base + j, 0], p], axis=0)
        total = dot(own[j, :, :B], p, NN) + dot(left, right, NN)
        blk[base + j] = (total + buf[base + j, 2].astype(F32)).astype(BF)
    for j in range(ranks):
        copy(base + j).start()
    for j in range(ranks):
        item = items[first + base + j]
        r = even[pl.ds(item, 1)] + letters[pl.ds(recvs[item], 1)]
        held[j : j + 1] = r
    for j in range(ranks):
        r = held[j : j + 1]
        c = THETA * r
        c = c + THETA * (r - joined(dot(split(c), blk[base + j], NT)))
        held[ranks + j : ranks + j + 1] = c
    for j in range(ranks):
        c = held[ranks + j : ranks + j + 1]
        held[2 * ranks + j : 2 * ranks + j + 1] = joined(dot(split(c), own[j, :, 2 * B :], NT))
    for j in range(ranks):
        item = items[first + base + j]
        restricted[pl.ds(item, 1)] = held[j : j + 1]
        reply[pl.ds(recvs[item], 1)] = held[ranks + j : ranks + j + 1]
        lift[pl.ds(item, 1)] = held[2 * ranks + j : 2 * ranks + j + 1]

    @pl.when(last)
    def _():
        for at in range(blk.shape[0]):
            copy(at).wait()


def early_kernel(ranks, early, items, recvs, starts, mail, even, own, *rest):
    parts = rest[:-11]
    blocks, rest_out, restricted, reply, lift, buf, blk, sem, part_sem, letters, held = rest[-11:]
    i = pl.program_id(0)

    def near(k):
        return pltpu.make_async_copy(
            parts[k], buf.at[pl.ds(starts[k], ranks)], part_sem.at[k]
        )

    @pl.when(i == 0)
    def _():
        for step in ("start", "wait"):
            for k in range(len(parts)):

                @pl.when(starts[k] >= 0)
                def _():
                    getattr(near(k), step)()

        rest_out[...] = buf[early:]
        letters[...] = mail[...].astype(F32)
        reply[...] = jnp.zeros_like(reply)
        restricted[...] = jnp.zeros_like(restricted)
        lift[...] = jnp.zeros_like(lift)

    last = i == pl.num_programs(0) - 1
    coarse_rows(i, 0, ranks, items, recvs, even, own, buf, blk, sem, letters, blocks, restricted, reply, lift, held, last)


def late_kernel(ranks, early, seen, items, recvs, starts, mail, even, own, before_r, before_y, before_l, blocks_in, rest_in, *rest):
    parts = rest[:-10]
    blocks, restricted, packed, lift, buf, blk, sem, part_sem, letters, held_all = rest[-10:]
    reply, held = held_all.at[pl.ds(0, letters.shape[0])], held_all.at[pl.ds(letters.shape[0], 4 * ranks)]
    i = pl.program_id(0)
    groups = buf.shape[0] // ranks

    def fresh(k):
        return pltpu.make_async_copy(
            parts[k - seen], buf.at[pl.ds(starts[k] - early, ranks)], part_sem.at[k]
        )

    def kept(k):
        at = pl.ds(starts[k] - early, ranks)
        return pltpu.make_async_copy(rest_in.at[at], buf.at[at], part_sem.at[k])

    @pl.when(i == 0)
    def _():
        for step in ("start", "wait"):
            for k in range(early // ranks, seen + len(parts)):

                @pl.when(starts[k] >= early)
                def _():
                    getattr(kept(k) if k < seen else fresh(k), step)()

        letters[...] = mail[...].astype(F32)
        reply[...] = before_y[...]
        restricted[...] = before_r[...]
        lift[...] = before_l[...]

    last = i == groups - 1
    coarse_rows(i, early, ranks, items, recvs, even, own, buf, blk, sem, letters, blocks, restricted, reply, lift, held, last)

    @pl.when(last)
    def _():
        packed[...] = reply[...].astype(BF)


def coarse_early(items, recvs, starts, ranks, early, parts, mail, even, own):
    half = even.shape[0]
    anywhere = pl.BlockSpec(memory_space=pl.ANY)
    return pl.pallas_call(
        functools.partial(early_kernel, ranks, early),
        out_shape=(
            jax.ShapeDtypeStruct((half, B, B), BF),
            jax.ShapeDtypeStruct((half - early, 3, B, B), BF),
            jax.ShapeDtypeStruct((half, B), F32),
            jax.ShapeDtypeStruct((2 * half, B), F32),
            jax.ShapeDtypeStruct((half, B), F32),
        ),
        grid_spec=pltpu.PrefetchScalarGridSpec(
            num_scalar_prefetch=3,
            grid=(early // ranks,),
            in_specs=[
                whole((2 * half, B)),
                whole((half, B)),
                pl.BlockSpec((ranks, B, 3 * B), lambda i, *_: (i, 0, 0)),
            ]
            + [anywhere] * len(parts),
            out_specs=(
                anywhere,
                whole((half - early, 3, B, B)),
                whole((half, B)),
                whole((2 * half, B)),
                whole((half, B)),
            ),
            scratch_shapes=[
                pltpu.VMEM((half, 3, B, B), BF),
                pltpu.VMEM((early, B, B), BF),
                pltpu.SemaphoreType.DMA((early,)),
                pltpu.SemaphoreType.DMA((len(parts),)),
                pltpu.VMEM((2 * half, B), F32),
                pltpu.VMEM((4 * ranks, B), F32),
            ],
        ),
        compiler_params=params(),
        name="coarse_early",
    )(items, recvs, starts, mail, even, own, *parts)


def coarse_late(items, recvs, starts, ranks, early, seen, parts, mail, even, own, restricted, reply, lift, blocks, kept):
    half = even.shape[0]
    late = half - early
    anywhere = pl.BlockSpec(memory_space=pl.ANY)
    return pl.pallas_call(
        functools.partial(late_kernel, ranks, early, seen),
        out_shape=(
            jax.ShapeDtypeStruct((half, B, B), BF),
            jax.ShapeDtypeStruct((half, B), F32),
            jax.ShapeDtypeStruct((2 * half, B), BF),
            jax.ShapeDtypeStruct((half, B), F32),
        ),
        grid_spec=pltpu.PrefetchScalarGridSpec(
            num_scalar_prefetch=3,
            grid=(late // ranks,),
            in_specs=[
                whole((2 * half, B)),
                whole((half, B)),
                pl.BlockSpec((ranks, B, 3 * B), lambda i, *_: (i + early // ranks, 0, 0)),
                whole((half, B)),
                whole((2 * half, B)),
                whole((half, B)),
                anywhere,
                anywhere,
            ]
            + [anywhere] * len(parts),
            out_specs=(anywhere, whole((half, B)), whole((2 * half, B)), whole((half, B))),
            scratch_shapes=[
                pltpu.VMEM((late, 3, B, B), BF),
                pltpu.VMEM((late, B, B), BF),
                pltpu.SemaphoreType.DMA((late,)),
                pltpu.SemaphoreType.DMA((seen + len(parts),)),
                pltpu.VMEM((2 * half, B), F32),
                pltpu.VMEM((2 * half + 4 * ranks, B), F32),
            ],
        ),
        input_output_aliases={9: 0},
        compiler_params=params(),
        name="coarse_late",
    )(items, recvs, starts, mail, even, own, restricted, reply, lift, blocks, kept, *parts)


def finish_kernel(group, sends, mail, lift, x, prol, out, letters):
    i = pl.program_id(0)

    @pl.when(i == 0)
    def _():
        letters[...] = mail[...].astype(F32)

    for j in range(group):
        e = 2 * j
        out[e : e + 1] = x[e : e + 1] + lift[j : j + 1]
        c = letters[pl.ds(sends[i * group + j], 1)]
        out[e + 1 : e + 2] = x[e + 1 : e + 2] + joined(dot(single(c), prol[j, 0], NT))


def finish(sends, mail, lift, x, prol, group=32):
    half = lift.shape[0]
    return pl.pallas_call(
        functools.partial(finish_kernel, group),
        out_shape=jax.ShapeDtypeStruct((2 * half, B), F32),
        grid_spec=pltpu.PrefetchScalarGridSpec(
            num_scalar_prefetch=1,
            grid=(half // group,),
            in_specs=[
                whole((2 * half, B)),
                pl.BlockSpec((group, B), lambda i, *_: (i, 0)),
                pl.BlockSpec((2 * group, B), lambda i, *_: (i, 0)),
                pl.BlockSpec((group, 1, B, B), lambda i, *_: (i, 1, 0, 0)),
            ],
            out_specs=pl.BlockSpec((2 * group, B), lambda i, *_: (i, 0)),
            scratch_shapes=[pltpu.VMEM((2 * half, B), F32)],
        ),
        compiler_params=params(),
        name="finish",
    )(sends, mail, lift, x, prol.reshape(half, 2, B, B))


def along(side, dx, dy):
    return [
        (x * side + y, (x + dx) % side * side + (y + dy) % side)
        for x in range(side)
        for y in range(side)
    ]


def gather_line(block):
    line = lax.axis_size("rx")
    copies = jnp.broadcast_to(block, (line,) + block.shape)
    gathered = lax.all_to_all(copies, "rx", split_axis=0, concat_axis=0, tiled=True)
    return gathered.reshape(-1, B)


def neighbours(block):
    count = lax.axis_size("ry")
    forward = [(i, (i + 1) % count) for i in range(count)]
    backward = [(target, source) for source, target in forward]
    return lax.ppermute(block, "ry", forward), lax.ppermute(block, "ry", backward)


def exchange(packed):
    line = lax.axis_size("rx")
    shape = packed.shape
    out = lax.all_to_all(
        packed.reshape((line, -1) + shape[1:]), "rx", split_axis=0, concat_axis=0, tiled=True
    )
    return out.reshape(shape)


def body(rhs, a_diag, a_pair, a_far, approx_inv, prolong, col_index, partner, odd_owner):
    rows = rhs.shape[0]
    half = rows // 2
    line_size = lax.axis_size("rx")
    side_size = lax.axis_size("ry")
    line_pos = lax.axis_index("rx")
    side_pos = lax.axis_index("ry")
    grid_side = 4
    capacity = half // (line_size // 2)
    mate = jnp.stack([partner, 2 * odd_owner], axis=1).reshape(rows)

    def line_slot(global_row):
        return global_row // rows // side_size * rows + global_row % rows

    side_dev = col_index[:, 1] // rows
    below = side_dev % side_size == (side_pos - 1) % side_size
    side_slot = jnp.where(below, 0, rows) + col_index[:, 1] % rows
    slots = jnp.concatenate([line_slot(mate), line_slot(col_index[:, 0]), side_slot])

    item_ids = jnp.arange(half, dtype=jnp.int32)
    codes = jnp.array([dx * grid_side + dy for dx, dy in ORDER], jnp.int32)[:, None]
    turns = jnp.arange(len(ORDER), dtype=jnp.int32)[:, None]

    def turn_of(line, ahead):
        dx = ahead * (line // grid_side - line_pos // grid_side) % grid_side
        dy = ahead * (line - line_pos) % grid_side
        hits = (dx * grid_side + dy)[None, :] == codes
        return jnp.sum(jnp.where(hits, turns, 0), axis=0, dtype=jnp.int32)

    def places_of(turn, rank):
        slot = turn * capacity + rank
        places = jnp.sum(slot[None, :] < slot[:, None], axis=1, dtype=jnp.int32)
        starts = jnp.sum(turn[None, :] < turns, axis=1, dtype=jnp.int32)
        used = jnp.any(turn[None, :] == turns, axis=1)
        return places, jnp.where(used, starts, -1)

    target_line = odd_owner // half // side_size
    same_target = target_line[:, None] == target_line[None, :]
    earlier = odd_owner[None, :] < odd_owner[:, None]
    send_rank = jnp.sum(same_target & earlier, axis=1, dtype=jnp.int32)
    sends = target_line * capacity + send_rank
    send_places, send_starts = places_of(turn_of(target_line, 1), send_rank)
    source_line = partner // rows // side_size
    same_source = source_line[:, None] == source_line[None, :]
    before = item_ids[None, :] < item_ids[:, None]
    recv_rank = jnp.sum(same_source & before, axis=1, dtype=jnp.int32)
    recvs = source_line * capacity + recv_rank
    recv_places, recv_starts = places_of(turn_of(source_line, -1), recv_rank)

    hits = recv_places[None, :] == item_ids[:, None]
    items = jnp.sum(jnp.where(hits, item_ids[None, :], 0), axis=1, dtype=jnp.int32)

    leaving = odd_blocks(send_places, send_starts, capacity, prolong, a_diag, a_pair)
    arrived = []

    def leave(first, last, gate):
        wait = max(first - WINDOW, 0)
        ins, old, gate = lax.optimization_barrier((leaving[first:last], arrived[wait:], gate))
        arrived[wait:] = old
        for part, (dx, dy) in zip(ins, ORDER[first:last]):
            arrived.append(lax.ppermute(part, "rx", along(grid_side, dx, dy)))
        return gate

    rhs = leave(0, 4, rhs)
    x, x_low = first_sweep(rhs, approx_inv)
    low, high = neighbours(x_low)
    table = gather_line(x_low)
    table = leave(4, 8, table)
    x, x_low = second_sweep(
        slots, rhs, x, table, low, high, a_diag, a_pair, a_far, approx_inv
    )
    low, high = neighbours(x_low)
    table = gather_line(x_low)
    table = leave(8, 13, table)
    own = even_blocks(recv_places, prolong, a_diag, a_pair)
    even, mail = residual_pieces(
        slots, sends, rhs, x, table, low, high, a_diag, a_pair, a_far, prolong
    )
    mail = exchange(mail)
    mail = leave(13, 15, mail)
    late = 2 * capacity
    early = half - late
    blocks, kept, restricted, reply, lift = coarse_early(
        items, recvs, recv_starts, capacity, early, arrived[:13], mail, even, own
    )
    blocks, restricted, reply, lift = coarse_late(
        items, recvs, recv_starts, capacity, early, 13, arrived[13:], mail, even, own, restricted, reply, lift, blocks, kept
    )
    fine = finish(sends, exchange(reply), lift, x, prolong)
    return fine, blocks, restricted


def solution(mesh):
    rows = P(("rx", "ry"))
    return jax.shard_map(
        body,
        mesh=mesh,
        in_specs=(rows,) * 9,
        out_specs=(rows,) * 3,
        check_vma=False,
    )
```
